128 devices in a mesh: gx: 4 (over x), gy: 4 (over z_hi, core), gz: 8 (over y, z_lo).
Axes of the slice: x: 4, y: 4, z: 4 (z_hi: 2, z_lo: 2; z = z_hi * 2 + z_lo), core: 2. Of those that a mesh axis runs over, the one named last changes fastest.
Arguments:
- amplitudes: bfloat16 [2, 65536, 2048], P(None, ('gx', 'gy', 'gz')), may hold values from -6 to 6
- pauli_x: int32 [200], replicated, may hold values from 0 to 2047, as said below
- pauli_z: int32 [200], replicated, may hold values from 0 to 2047
- pauli_phase: int32 [200], replicated, may hold values from 0 to 3
Outputs:
- density_real: float32 [2048, 2048], P(('gx', 'gy', 'gz'))
- density_imag: float32 [2048, 2048], P(('gx', 'gy', 'gz'))
- expectations: float32 [2, 200], replicated
The draws below stay inside these ranges and needn't reach their ends.
Inputs may be any that keep to these rules, and one draw needn't show every extreme that they name: Bit q of the mask acts on kept qubit q (the bit of weight 2^q of the last index); pauli_x and pauli_z of a term are never both zero.
All inputs are finite; a program needn't handle non-finite values.
Results may differ from the reference program's by a relative error of at most 0.0003.
Values sent between devices are 32-bit elements; how exact they have to be, the bound alone decides.
A program may use at most 192 MiB of HBM per device.

```python
import jax
import jax.numpy as jnp
from jax import lax

QUBITS = 11
R = 2048
COLS_ALL = 65536
TERMS = 200


def pauli_masks(key):
    flips = jax.random.randint(jax.random.fold_in(key, 11), (TERMS,), 0, R).astype(jnp.int32)
    phases = jax.random.randint(jax.random.fold_in(key, 23), (TERMS,), 0, R).astype(jnp.int32)
    both_zero = jnp.logical_and(flips == 0, phases == 0)
    phases = jnp.where(both_zero, jnp.int32(1), phases)
    return (flips, phases)


def draw_pauli_x(key, part):
    return pauli_masks(key)[0]


def draw_pauli_z(key, part):
    return pauli_masks(key)[1]


def with_ends(result, key, low, top_value):
    shape = result.shape
    index_at = [jax.random.randint(jax.random.fold_in(key, axis), (), 0, shape[axis]) for axis in range(len(shape))]
    result = result.at[tuple(index_at)].set(low)
    longest = shape.index(max(shape))
    index_at[longest] = (index_at[longest] + 1) % shape[longest]
    return result.at[tuple(index_at)].set(top_value)


def shard_levels(key, extent, cuts, low, high):
    gain, own = 1.0, jax.random.fold_in(key, 6)
    for position, parts in cuts:
        heights = jnp.exp(jax.random.uniform(jax.random.fold_in(own, position), (parts,), jnp.float32, low / len(cuts), high / len(cuts)))
        gain = gain * jnp.repeat(heights, extent[position] // parts).reshape([-1 if axis == position else 1 for axis in range(len(extent))])
    return gain


def bell_draw(stream_key, extent, width, limit, shards=(), kind=jnp.bfloat16):
    array = width * jax.random.normal(stream_key, extent, jnp.float32)
    if shards:
        array = array * shard_levels(stream_key, extent, shards, -0.22, 0.18)
    return jnp.clip(array, -limit, limit).astype(kind)


def setup_inputs(seed: int = 0) -> dict:
    streams_of = jax.random.split(jax.random.key(seed), 5)
    return {
        "amplitudes": bell_draw(streams_of[0], (2, COLS_ALL, R), 1.0, 6.0, ((1, 128),)),
        "pauli_x": draw_pauli_x(jax.random.fold_in(streams_of[4], 71), 0),
        "pauli_z": draw_pauli_z(jax.random.fold_in(streams_of[4], 71), 0),
        "pauli_phase": with_ends(jax.random.randint(streams_of[3], (TERMS,), 0, 4), jax.random.fold_in(streams_of[3], 1), 0, 3).astype(jnp.int32),
    }


def parity_sign(values, masks):
    anded = jnp.bitwise_and(values, masks)
    counted = jnp.zeros_like(anded)
    for bit_index in range(QUBITS):
        counted = counted + jnp.bitwise_and(jnp.right_shift(anded, bit_index), 1)
    return (1 - 2 * jnp.bitwise_and(counted, 1)).astype(jnp.float32)


def phase_parts(pauli_phase):
    phase_real = jnp.where(pauli_phase == 0, 1.0, jnp.where(pauli_phase == 2, -1.0, 0.0)).astype(jnp.float32)
    phase_imag = jnp.where(pauli_phase == 1, 1.0, jnp.where(pauli_phase == 3, -1.0, 0.0)).astype(jnp.float32)
    return phase_real, phase_imag


def reference(amplitudes, pauli_x, pauli_z, pauli_phase):
    real_part = amplitudes[0].astype(jnp.float32)
    imag_part = amplitudes[1].astype(jnp.float32)
    dims = (((0,), (0,)), ((), ()))
    high = lax.Precision.HIGHEST
    gram_real = lax.dot_general(real_part, real_part, dims, precision=high) + lax.dot_general(imag_part, imag_part, dims, precision=high)
    gram_imag = lax.dot_general(imag_part, real_part, dims, precision=high) - lax.dot_general(real_part, imag_part, dims, precision=high)
    total_cols = amplitudes.shape[1]
    density_real = gram_real / total_cols
    density_imag = gram_imag / total_cols
    row_ids = jnp.arange(R, dtype=jnp.int32)[None, :]
    partner = jnp.bitwise_xor(row_ids, pauli_x[:, None])
    picked_real = jnp.take_along_axis(density_real, partner.T, axis=1).T
    picked_imag = jnp.take_along_axis(density_imag, partner.T, axis=1).T
    signs = parity_sign(row_ids, pauli_z[:, None])
    phase_real, phase_imag = phase_parts(pauli_phase)
    sum_real = jnp.sum(signs * picked_real, axis=1)
    sum_imag = jnp.sum(signs * picked_imag, axis=1)
    expect_real = phase_real * sum_real - phase_imag * sum_imag
    expect_imag = phase_real * sum_imag + phase_imag * sum_real
    return density_real, density_imag, jnp.stack([expect_real, expect_imag], 0)
```

```python
import functools

import jax
import jax.numpy as jnp
from jax import lax
from jax.experimental import pallas as pl
from jax.experimental.pallas import tpu as pltpu
from jax.sharding import Mesh
from jax.sharding import PartitionSpec as P

ORDER = 2048
COLS = 65536
DEPTH = 512
TERMS = 200
TERMS_PAD = 256
AXES = ("gx", "gy_0", "gy_1", "gz_0", "gz_1")
ROWS = (slice(0, 88), slice(88, 176), slice(176, 256))
ROW_HALVES = (
    (slice(0, 48), slice(48, 88)),
    (slice(88, 136), slice(136, 176)),
    (slice(176, 216), slice(216, 256)),
)
FAR, PURE, ACC = 0, 1, 2
LAG = 4
LO, HI = slice(0, 2), slice(2, 4)
HALF = (LO, HI)


def offset(r):
    return lax.rem(2 + r + r // 2 + 2 * (r // 3), 4)


def remote(src, dst, send, recv, device):
    return pltpu.make_async_remote_copy(
        src_ref=src,
        dst_ref=dst,
        send_sem=send,
        recv_sem=recv,
        device_id=device,
        device_id_type=pl.DeviceIdType.MESH,
    )


def parity(values):
    values = values ^ (values >> 8)
    values = values ^ (values >> 4)
    values = values ^ (values >> 2)
    values = values ^ (values >> 1)
    return values & 1


def kernel(
    amp, px, pz, pph,
    out_re, out_im, out_ex,
    s, t, p, stage, cross, ph1, ph2, ph3, flipped, direct, mirror, part,
    in_sem, core_ss, core_rs, ss1, rs1, ss2, rs2, ss3, rs3,
    dss, drs, mss, mrs, ess, ers,
):
    x0 = lax.axis_index("gx")
    zh = lax.axis_index("gy_0")
    core = lax.axis_index("gy_1")
    y0 = lax.axis_index("gz_0")
    zl = lax.axis_index("gz_1")
    z0 = 2 * zh + zl
    me = x0 * 32 + zh * 16 + core * 8 + y0 * 2 + zl

    def at_x(step):
        return {"gx": lax.rem(x0 + step, 4)}

    def at_y(step):
        return {"gz_0": lax.rem(y0 + step, 4)}

    def at_z(step):
        z = lax.rem(z0 + step, 4)
        return {"gy_0": z // 2, "gz_1": lax.rem(z, 2)}

    along = (at_x, at_y, at_z)
    other_core = {"gy_1": 1 - core}

    load = pltpu.make_async_copy(amp, s, in_sem)
    load.start()
    barrier = pltpu.get_barrier_semaphore()
    partners = [other_core] + [f(k) for f in along for k in (1, 3)]
    for device in partners:
        pl.semaphore_signal(barrier, inc=1, device_id=device, device_id_type=pl.DeviceIdType.MESH)
    pl.semaphore_wait(barrier, len(partners))
    load.wait()

    def transposed(slot, block):
        first = pl.multiple_of(block * 256, 256)
        re_t = s[0, :, pl.ds(first, 256)].T
        im_t = s[1, :, pl.ds(first, 256)].T
        t[slot, 0] = re_t
        t[slot, 1] = im_t
        t[slot, 2] = -re_t

    def block_product(slot, block, y, x, half, dst):
        col = 2 * x + half
        first = pl.multiple_of(col * 256, 256)

        def product(k):
            return jnp.dot(
                t[slot, k], s[0, :, pl.ds(first, 256)], preferred_element_type=jnp.float32
            ) + jnp.dot(
                t[slot, k + 1], s[1, :, pl.ds(first, 256)], preferred_element_type=jnp.float32
            )

        def put(value):
            dst[y, x, 2 * half] = value[:, :128]
            dst[y, x, 2 * half + 1] = value[:, 128:]

        @pl.when(block != col)
        def _():
            put(product((block - col + 8) // 8))

        @pl.when(block == col)
        def _():
            row = lax.broadcasted_iota(jnp.int32, (256, 256), 0)
            lane = lax.broadcasted_iota(jnp.int32, (256, 256), 1)
            put(jnp.where(lane >= row, product(0), product(1)))

    def unit_of(v):
        off_y, off_x = offset(v // 4), offset(lax.rem(v, 4))
        return off_y, off_x, lax.rem(y0 + off_y, 4), lax.rem(x0 + off_x, 4)

    def core_copy(v, y, x):
        return remote(stage.at[y, x], cross.at[y, x], core_ss.at[v], core_rs.at[v], other_core)

    def send1(kind, o, src, key, index, step):
        remote(
            src,
            ph1.at[(kind,) + key + (ROWS[o],)],
            ss1.at[kind, o, index],
            rs1.at[kind, o, index],
            along[o](step),
        ).start()

    def wait1(kind, o, key, index):
        ref = ph1.at[(kind,) + key + (ROWS[o],)]
        remote(ref, ref, ss1.at[kind, o, index], rs1.at[kind, o, index], along[o](1)).wait_recv()

    def finish(v):
        off_y, off_x, y, x = unit_of(v)
        core_copy(v, y, x).wait_recv()
        for z in range(4):
            p[y, x, z] += cross[y, x, z]
        for o, off, line in ((0, off_x, y), (1, off_y, x)):
            @pl.when(off == 2)
            def _(o=o, line=line):
                for h, step in ((0, 1), (1, 3)):
                    send1(FAR, o, p.at[y, x, HALF[h], ROWS[o]], (line, HALF[h]), 2 * line + h, step)

            @pl.when(off == 1)
            def _(o=o, line=line):
                send1(PURE, o, p.at[y, x, HI, ROWS[o]], (line, HI), 2 * line + 1, 1)

            @pl.when(off == 3)
            def _(o=o, line=line):
                send1(PURE, o, p.at[y, x, LO, ROWS[o]], (line, LO), 2 * line, 3)

        up = lax.rem(v, 2)
        far, right, left = (lax.rem(z0 + k, 4) for k in (2, 1, 3))

        @pl.when(up == 0)
        def _():
            send1(FAR, 2, p.at[y, x, far, ROWS[2]], (y, x), 4 * y + x, 1)
            send1(PURE, 2, p.at[y, x, left, ROWS[2]], (y, x), 4 * y + x, 3)

        @pl.when(up == 1)
        def _():
            send1(FAR, 2, p.at[y, x, far, ROWS[2]], (y, x), 4 * y + x, 3)
            send1(PURE, 2, p.at[y, x, right, ROWS[2]], (y, x), 4 * y + x, 1)

    def forward(v):
        off_y, off_x, y, x = unit_of(v)
        for o, off, line in ((0, off_x, y), (1, off_y, x)):
            for h, step in ((0, 1), (1, 3)):
                @pl.when(off == step)
                def _(o=o, line=line, h=h, step=step):
                    key, index = (line, HALF[h]), 2 * line + h
                    wait1(FAR, o, key, index)
                    p[y, x, HALF[h], ROWS[o]] += ph1[FAR, line, HALF[h], ROWS[o]]
                    send1(ACC, o, p.at[y, x, HALF[h], ROWS[o]], key, index, step)

        wait1(FAR, 2, (y, x), 4 * y + x)
        for h, step in ((0, 1), (1, 3)):
            @pl.when(lax.rem(v, 2) == h)
            def _(step=step):
                z = lax.rem(z0 + step, 4)
                p[y, x, z, ROWS[2]] += ph1[FAR, y, x, ROWS[2]]
                send1(ACC, 2, p.at[y, x, z, ROWS[2]], (y, x), 4 * y + x, step)

    def step(u, carry):
        _, _, y, x = unit_of(u)

        @pl.when(lax.rem(u, 4) == 0)
        def _():
            transposed(0, 4 * (1 - core) + y)
            transposed(1, 4 * core + y)

        for half in range(2):
            block_product(0, 4 * (1 - core) + y, y, x, half, stage)
        core_copy(u, y, x).start()
        for half in range(2):
            block_product(1, 4 * core + y, y, x, half, p)

        @pl.when(u >= 1)
        def _():
            finish(u - 1)

        @pl.when(u >= 1 + LAG)
        def _():
            forward(u - 1 - LAG)

        return carry

    lax.fori_loop(0, 16, step, 0)
    finish(15)
    lax.fori_loop(15 - LAG, 16, lambda v, carry: (forward(v), carry)[1], 0)

    def held(o, b, cs):
        if o == 0:
            return (b, x0, cs, ROWS[0])
        if o == 1:
            return (y0, cs, b, ROWS[1])
        return (cs, b, z0, ROWS[2])

    def landed(o, b, cs):
        return (b, cs, ROWS[0]) if o == 0 else (cs, b, ROWS[o])

    origin2 = (y0, z0, x0)
    origin3 = (z0, x0, y0)
    along2 = (at_y, at_z, at_x)
    along3 = (at_z, at_x, at_y)
    every = slice(0, 4)

    def take1(o, b, first):
        if o == 0:
            for kind in (PURE, ACC):
                for h in range(2):
                    wait1(kind, 0, (b, HALF[h]), 2 * b + h)
        elif o == 1:
            if first:
                for kind in (PURE, ACC):
                    for line in range(4):
                        for h in range(2):
                            wait1(kind, 1, (line, HALF[h]), 2 * line + h)
        else:
            for kind in (PURE, ACC):
                for y in range(4):
                    wait1(kind, 2, (y, b), 4 * y + b)
        for c in range(4):
            p[held(o, b, c)] += ph1[(PURE,) + landed(o, b, c)] + ph1[(ACC,) + landed(o, b, c)]

    def copy2(kind, o, src, h, step):
        return remote(
            src, ph2.at[kind, HALF[h], ROWS[o]], ss2.at[kind, o, h], rs2.at[kind, o, h],
            along2[o](step),
        )

    def wait2(kind, o, h):
        copy2(kind, o, ph2.at[kind, HALF[h], ROWS[o]], h, 1).wait_recv()

    def at2(o, k):
        return lax.rem(origin2[o] + k, 4)

    for o in range(3):
        b = at2(o, 2)
        take1(o, b, True)
        for h, step in ((0, 1), (1, 3)):
            copy2(FAR, o, p.at[held(o, b, HALF[h])], h, step).start()
    for o in range(3):
        for h, step in ((1, 1), (0, 3)):
            b = at2(o, step)
            take1(o, b, False)
            copy2(PURE, o, p.at[held(o, b, HALF[h])], h, step).start()
    for o in range(3):
        for h, step in ((0, 1), (1, 3)):
            b = at2(o, step)
            wait2(FAR, o, h)
            p[held(o, b, HALF[h])] += ph2[FAR, HALF[h], ROWS[o]]
            copy2(ACC, o, p.at[held(o, b, HALF[h])], h, step).start()
    for o in range(3):
        take1(o, origin2[o], False)

    def own(o, c, rows):
        return held(o, origin2[o], c)[:3] + (rows,)

    def copy3(kind, o, src, h, step):
        return remote(
            src, ph3.at[kind, ROW_HALVES[o][h]], ss3.at[kind, o, h], rs3.at[kind, o, h],
            along3[o](step),
        )

    def wait3(kind, o, h):
        copy3(kind, o, ph3.at[kind, ROW_HALVES[o][h]], h, 1).wait_recv()

    def take2(o, c):
        p[own(o, c, ROWS[o])] += ph2[PURE, c, ROWS[o]] + ph2[ACC, c, ROWS[o]]

    def at3(o, k):
        return lax.rem(origin3[o] + k, 4)

    for o in range(3):
        for kind in (PURE, ACC):
            for h in range(2):
                wait2(kind, o, h)
        c = at3(o, 2)
        take2(o, c)
        for h, step in ((0, 1), (1, 3)):
            copy3(FAR, o, p.at[own(o, c, ROW_HALVES[o][h])], h, step).start()
    for o in range(3):
        for h, step in ((1, 1), (0, 3)):
            c = at3(o, step)
            take2(o, c)
            copy3(PURE, o, p.at[own(o, c, ROW_HALVES[o][h])], h, step).start()
    for o in range(3):
        for h, step in ((0, 1), (1, 3)):
            c = at3(o, step)
            wait3(FAR, o, h)
            p[own(o, c, ROW_HALVES[o][h])] += ph3[FAR, ROW_HALVES[o][h]]
            copy3(ACC, o, p.at[own(o, c, ROW_HALVES[o][h])], h, step).start()
    for o in range(3):
        take2(o, origin3[o])
    for o in range(3):
        for kind in (PURE, ACC):
            for h in range(2):
                wait3(kind, o, h)
    block = p[y0, x0, z0] + ph3[PURE] + ph3[ACC]
    p[y0, x0, z0] = block
    flipped[...] = block.T

    row_block = 4 * core + y0
    col_block = 4 * x0 + z0

    def device(e):
        return {
            "gx": e // 32,
            "gy_0": lax.rem(e // 16, 2),
            "gy_1": lax.rem(e // 8, 2),
            "gz_0": lax.rem(e // 2, 4),
            "gz_1": lax.rem(e, 2),
        }

    def direct_copy(k):
        e = 16 * row_block + k
        return e, remote(
            p.at[y0, x0, z0, pl.ds(16 * k, 16)], direct.at[col_block],
            dss.at[k], drs.at[col_block], device(e),
        )

    def mirror_copy(k):
        e = 8 * col_block + k
        return e, remote(
            flipped.at[pl.ds(16 * k, 16)], mirror.at[row_block],
            mss.at[k], mrs.at[row_block], device(e),
        )

    for k in range(16):
        e, copy = direct_copy(k)

        @pl.when(e != me)
        def _(copy=copy):
            copy.start()

        @pl.when(e == me)
        def _(k=k):
            direct[col_block] = p[y0, x0, z0, pl.ds(16 * k, 16)]

    for k in range(8):
        e, copy = mirror_copy(k)

        @pl.when(e != me)
        def _(copy=copy):
            copy.start()

        @pl.when(e == me)
        def _(k=k):
            mirror[row_block] = flipped[pl.ds(16 * k, 16)]

    row = lax.broadcasted_iota(jnp.int32, (256, 128), 0)
    lane = lax.broadcasted_iota(jnp.int32, (256, 128), 1)
    moved = block
    for bit in range(7):
        hop = 1 << bit
        swapped = jnp.where(
            (lane & hop) != 0, pltpu.roll(moved, hop, 1), pltpu.roll(moved, 128 - hop, 1)
        )
        moved = jnp.where((row & hop) != 0, swapped, moved)
    in_row = 256 * row_block + row
    in_col = 128 * col_block + ((row & 127) ^ lane)
    upper = jnp.where(in_col >= in_row, moved, 0.0)
    lower = jnp.where(in_col >= in_row, 0.0, moved)
    xs, zs, phase = px[...], pz[...], pph[...]
    pick_row = lax.broadcasted_iota(jnp.int32, (128, TERMS), 0)
    pick = jnp.where(pick_row == (xs & 127), 1.0, 0.0).astype(jnp.float32)
    dot = functools.partial(
        jnp.dot, preferred_element_type=jnp.float32, precision=lax.Precision.HIGHEST
    )
    term_row = 256 * row_block + lax.broadcasted_iota(jnp.int32, (256, TERMS), 0)
    sign = (1 - 2 * parity(term_row & zs)).astype(jnp.float32)
    sign = jnp.where(((term_row >> 7) ^ (xs >> 7)) == col_block, sign, 0.0)
    even = (1 - parity(xs & zs)).astype(jnp.float32)
    real_weight = jnp.where(xs == 0, 1.0, 2.0 * even)
    imag_weight = 2.0 - 2.0 * even
    sum_re = real_weight * jnp.sum(sign * dot(upper, pick), axis=0, keepdims=True)
    sum_im = imag_weight * jnp.sum(sign * dot(lower, pick), axis=0, keepdims=True)
    phase_re = jnp.where(phase == 0, 1.0, jnp.where(phase == 2, -1.0, 0.0))
    phase_im = jnp.where(phase == 1, 1.0, jnp.where(phase == 3, -1.0, 0.0))
    scale = 1.0 / COLS
    here = jnp.concatenate(
        [
            (phase_re * sum_re - phase_im * sum_im) * scale,
            (phase_re * sum_im + phase_im * sum_re) * scale,
            jnp.zeros((6, TERMS), jnp.float32),
        ],
        axis=0,
    )

    for stage_no, (mine, count, where) in enumerate(
        ((core, 2, lambda k: other_core), (x0, 4, at_x), (y0, 4, at_y), (z0, 4, at_z))
    ):
        part[stage_no, mine, :, :TERMS] = here
        for k in range(1, count):
            remote(
                part.at[stage_no, mine], part.at[stage_no, mine],
                ess.at[stage_no, k], ers.at[stage_no, mine], where(k),
            ).start()
        for k in range(1, count):
            source = lax.rem(mine + k, count)
            slot = part.at[stage_no, source]
            remote(
                slot, slot, ess.at[stage_no, k], ers.at[stage_no, source], where(k)
            ).wait_recv()
        here = part[stage_no, 0, :, :TERMS]
        for k in range(1, count):
            here = here + part[stage_no, k, :, :TERMS]
    out_ex[...] = here[:2]

    for k in range(16):
        sender_x, sender_z = k // 4, k % 4
        sender = (sender_x * 32 + (sender_z // 2) * 16 + (me // 64) * 8
                  + lax.rem(me // 16, 4) * 2 + sender_z % 2)

        @pl.when(sender != me)
        def _(k=k):
            ref = direct.at[k]
            remote(ref, ref, dss.at[0], drs.at[k], other_core).wait_recv()

    for k in range(8):
        sender_core, sender_y = k // 4, k % 4
        sender_x, sender_z = me // 32, lax.rem(me // 8, 4)
        sender = (sender_x * 32 + (sender_z // 2) * 16 + sender_core * 8
                  + sender_y * 2 + lax.rem(sender_z, 2))

        @pl.when(sender != me)
        def _(k=k):
            ref = mirror.at[k]
            remote(ref, ref, mss.at[0], mrs.at[k], other_core).wait_recv()

    row = 16 * me + lax.broadcasted_iota(jnp.int32, (16, 128), 0)
    lane = lax.broadcasted_iota(jnp.int32, (16, 128), 1)
    for k in range(16):
        given = direct[k] * scale
        turned = mirror[k // 2, :, 128 * (k % 2) : 128 * (k % 2) + 128] * scale
        col = 128 * k + lane
        out_re[:, 128 * k : 128 * k + 128] = jnp.where(col >= row, given, turned)
        out_im[:, 128 * k : 128 * k + 128] = jnp.where(
            col < row, given, jnp.where(col == row, 0.0, -turned)
        )

    def sent_unit(v, carry):
        _, _, y, x = unit_of(v)
        core_copy(v, y, x).wait_send()
        for kind in range(3):
            ref = ph1.at[kind, 0, 0, ROWS[2]]
            remote(ref, ref, ss1.at[kind, 2, v], rs1.at[kind, 2, v], at_z(1)).wait_send()
        return carry

    lax.fori_loop(0, 16, sent_unit, 0)

    def sent_pair(v, carry):
        for kind in range(3):
            for o in range(2):
                ref = ph1.at[kind, 0, LO, ROWS[o]]
                remote(ref, ref, ss1.at[kind, o, v], rs1.at[kind, o, v], at_x(1)).wait_send()
        return carry

    lax.fori_loop(0, 8, sent_pair, 0)
    for kind in range(3):
        for o in range(3):
            for h in range(2):
                copy2(kind, o, ph2.at[kind, HALF[h], ROWS[o]], h, 1).wait_send()
                copy3(kind, o, ph3.at[kind, ROW_HALVES[o][h]], h, 1).wait_send()
    for k in range(16):
        e, copy = direct_copy(k)

        @pl.when(e != me)
        def _(copy=copy):
            copy.wait_send()

    for k in range(8):
        e, copy = mirror_copy(k)

        @pl.when(e != me)
        def _(copy=copy):
            copy.wait_send()

    for stage_no, count in enumerate((2, 4, 4, 4)):
        for k in range(1, count):
            slot = part.at[stage_no, 0]
            remote(
                slot, slot, ess.at[stage_no, k], ers.at[stage_no, 0], other_core
            ).wait_send()


def on_device(amplitudes, pauli_x, pauli_z, pauli_phase):
    vmem = pl.BlockSpec(memory_space=pltpu.VMEM)
    f32 = jnp.float32
    dma = pltpu.SemaphoreType.DMA
    return pl.pallas_call(
        kernel,
        out_shape=(
            jax.ShapeDtypeStruct((16, ORDER), f32),
            jax.ShapeDtypeStruct((16, ORDER), f32),
            jax.ShapeDtypeStruct((2, TERMS), f32),
        ),
        in_specs=[pl.BlockSpec(memory_space=pl.ANY), vmem, vmem, vmem],
        out_specs=(vmem, vmem, vmem),
        scratch_shapes=[
            pltpu.VMEM((2, DEPTH, ORDER), jnp.bfloat16),
            pltpu.VMEM((2, 3, 256, DEPTH), jnp.bfloat16),
            pltpu.VMEM((4, 4, 4, 256, 128), f32),
            pltpu.VMEM((4, 4, 4, 256, 128), f32),
            pltpu.VMEM((4, 4, 4, 256, 128), f32),
            pltpu.VMEM((3, 4, 4, 256, 128), f32),
            pltpu.VMEM((3, 4, 256, 128), f32),
            pltpu.VMEM((3, 256, 128), f32),
            pltpu.VMEM((128, 256), f32),
            pltpu.VMEM((16, 16, 128), f32),
            pltpu.VMEM((8, 16, 256), f32),
            pltpu.VMEM((4, 4, 8, TERMS_PAD), f32),
            dma(()),
            dma((16,)),
            dma((16,)),
            dma((3, 3, 16)),
            dma((3, 3, 16)),
            dma((3, 3, 2)),
            dma((3, 3, 2)),
            dma((3, 3, 2)),
            dma((3, 3, 2)),
            dma((16,)),
            dma((16,)),
            dma((8,)),
            dma((8,)),
            dma((4, 4)),
            dma((4, 4)),
        ],
        compiler_params=pltpu.CompilerParams(
            collective_id=0, has_side_effects=True, vmem_limit_bytes=60 * 1024 * 1024
        ),
    )(amplitudes, pauli_x.reshape(1, TERMS), pauli_z.reshape(1, TERMS), pauli_phase.reshape(1, TERMS))


def solution(mesh):
    finer = Mesh(mesh.devices.reshape(mesh.shape["gx"], 2, 2, 4, 2), AXES)
    return jax.shard_map(
        on_device,
        mesh=finer,
        in_specs=(P(None, AXES, None), P(), P(), P()),
        out_specs=(P(AXES, None), P(AXES, None), P()),
        check_vma=False,
    )
```

```python
import functools

import jax
import jax.numpy as jnp
from jax import lax
from jax.experimental import pallas as pl
from jax.experimental.pallas import tpu as pltpu
from jax.sharding import Mesh
from jax.sharding import PartitionSpec as P

ORDER = 2048
COLS = 65536
DEPTH = 512
TERMS = 200
TERMS_PAD = 256
AXES = ("gx", "gy_0", "gy_1", "gz_0", "gz_1")
ROWS = (slice(0, 88), slice(88, 176), slice(176, 256))
FAR, PURE, ACC = 0, 1, 2
LAG = 3
BASE = (0, 8, 16)
LO, HI = slice(0, 2), slice(2, 4)
HALF = (LO, HI)


def offset(r):
    return lax.rem(2 + r + r // 2 + 2 * (r // 3), 4)


def remote(src, dst, send, recv, device):
    return pltpu.make_async_remote_copy(
        src_ref=src,
        dst_ref=dst,
        send_sem=send,
        recv_sem=recv,
        device_id=device,
        device_id_type=pl.DeviceIdType.MESH,
    )


def parity(values):
    values = values ^ (values >> 8)
    values = values ^ (values >> 4)
    values = values ^ (values >> 2)
    values = values ^ (values >> 1)
    return values & 1


def kernel(
    amp, px, pz, pph,
    out_re, out_im, out_ex,
    s, t, p, stage, cross, ph1, ph2, ph3, flipped, direct, mirror, weights, part0, part1,
    in_sem, core_ss, core_rs, ss1, rs1, ss2, rs2, ss3, rs3,
    dss, drs, mss, mrs, ess, ers,
):
    x0 = lax.axis_index("gx")
    zh = lax.axis_index("gy_0")
    core = lax.axis_index("gy_1")
    y0 = lax.axis_index("gz_0")
    zl = lax.axis_index("gz_1")
    z0 = 2 * zh + zl
    me = x0 * 32 + zh * 16 + core * 8 + y0 * 2 + zl

    def at_x(step):
        return {"gx": lax.rem(x0 + step, 4)}

    def at_y(step):
        return {"gz_0": lax.rem(y0 + step, 4)}

    def at_z(step):
        z = lax.rem(z0 + step, 4)
        return {"gy_0": z // 2, "gz_1": lax.rem(z, 2)}

    along = (at_x, at_y, at_z)
    along2 = (at_y, at_z, at_x)
    along3 = (at_z, at_x, at_y)
    origin2 = (y0, z0, x0)
    origin3 = (z0, x0, y0)
    other_core = {"gy_1": 1 - core}
    blocks = (4 * (1 - core), 4 * core)

    def transposed(slot, y):
        first = pl.multiple_of((blocks[slot] + y) * 256, 256)
        re_t = s[:DEPTH, pl.ds(first, 256)].T
        im_t = s[DEPTH:, pl.ds(first, 256)].T
        t[slot, :, :DEPTH] = re_t
        t[slot, :, DEPTH : 2 * DEPTH] = im_t
        t[slot, :, 2 * DEPTH :] = -re_t

    def factor(slot, imag):
        return t[slot, :, pl.ds(pl.multiple_of(imag * DEPTH, DEPTH), 2 * DEPTH)]

    def column(col):
        return s[:, pl.ds(pl.multiple_of(col * 256, 256), 256)]

    dot = functools.partial(jnp.dot, preferred_element_type=jnp.float32)

    def products(y, x):
        for half in range(2):
            col = 2 * x + half
            left = jnp.concatenate(
                [factor(slot, (blocks[slot] + y - col + 7) // 8) for slot in range(2)], axis=0
            )
            value = dot(left, column(col))
            for slot, dst in ((0, stage), (1, p)):
                for k in range(2):
                    dst[y, x, 2 * half + k] = value[
                        256 * slot : 256 * slot + 256, 128 * k : 128 * k + 128
                    ]

    def mend(y, x):
        for slot, dst in ((0, stage), (1, p)):
            block = blocks[slot] + y

            @pl.when(block // 2 == x)
            def _(slot=slot, dst=dst, block=block):
                imag = dot(factor(slot, 1), column(block))
                row = lax.broadcasted_iota(jnp.int32, (256, 128), 0)
                lane = lax.broadcasted_iota(jnp.int32, (256, 128), 1)
                for k in range(2):
                    z = 2 * lax.rem(block, 2) + k
                    dst[y, x, z] = jnp.where(
                        lane + 128 * k >= row, dst[y, x, z], imag[:, 128 * k : 128 * k + 128]
                    )

    def unit_of(v):
        off_y, off_x = offset(v // 4), offset(lax.rem(v, 4))
        return off_y, off_x, lax.rem(y0 + off_y, 4), lax.rem(x0 + off_x, 4)

    def core_copy(v, y, x):
        return remote(stage.at[y, x], cross.at[y, x], core_ss.at[0], core_rs.at[v], other_core)

    def copy1(kind, o, src, key, index, step):
        return remote(
            src,
            ph1.at[(kind,) + key + (ROWS[o],)],
            ss1.at[kind, o],
            rs1.at[kind, BASE[o] + index],
            along[o](step),
        )

    def send1(kind, o, src, key, index, step):
        copy1(kind, o, src, key, index, step).start()

    def wait1(kind, o, key, index):
        copy1(kind, o, ph1.at[(kind,) + key + (ROWS[o],)], key, index, 1).wait_recv()

    def add_cross(y, x):
        for z in range(4):
            p[y, x, z] += cross[y, x, z]

    def finish(v):
        off_y, off_x, y, x = unit_of(v)
        for o, off, line in ((0, off_x, y), (1, off_y, x)):
            @pl.when(off == 2)
            def _(o=o, line=line):
                for h, step in ((0, 1), (1, 3)):
                    send1(FAR, o, p.at[y, x, HALF[h], ROWS[o]], (line, HALF[h]), 2 * line + h, step)

            @pl.when(off == 1)
            def _(o=o, line=line):
                send1(PURE, o, p.at[y, x, HI, ROWS[o]], (line, HI), 2 * line + 1, 1)

            @pl.when(off == 3)
            def _(o=o, line=line):
                send1(PURE, o, p.at[y, x, LO, ROWS[o]], (line, LO), 2 * line, 3)

        up = lax.rem(v, 2)
        far, right, left = (lax.rem(z0 + k, 4) for k in (2, 1, 3))

        @pl.when(up == 0)
        def _():
            send1(FAR, 2, p.at[y, x, far, ROWS[2]], (y, x), 4 * y + x, 1)
            send1(PURE, 2, p.at[y, x, left, ROWS[2]], (y, x), 4 * y + x, 3)

        @pl.when(up == 1)
        def _():
            send1(FAR, 2, p.at[y, x, far, ROWS[2]], (y, x), 4 * y + x, 3)
            send1(PURE, 2, p.at[y, x, right, ROWS[2]], (y, x), 4 * y + x, 1)

    def forward(v):
        off_y, off_x, y, x = unit_of(v)
        for o, off, line in ((0, off_x, y), (1, off_y, x)):
            for h, step in ((0, 1), (1, 3)):
                @pl.when(off == step)
                def _(o=o, line=line, h=h, step=step):
                    key, index = (line, HALF[h]), 2 * line + h
                    wait1(FAR, o, key, index)
                    p[y, x, HALF[h], ROWS[o]] += ph1[FAR, line, HALF[h], ROWS[o]]
                    send1(ACC, o, p.at[y, x, HALF[h], ROWS[o]], key, index, step)

        wait1(FAR, 2, (y, x), 4 * y + x)
        for h, step in ((0, 1), (1, 3)):
            @pl.when(lax.rem(v, 2) == h)
            def _(step=step):
                z = lax.rem(z0 + step, 4)
                p[y, x, z, ROWS[2]] += ph1[FAR, y, x, ROWS[2]]
                send1(ACC, 2, p.at[y, x, z, ROWS[2]], (y, x), 4 * y + x, step)

    def held(o, b, cs):
        if o == 0:
            return (b, x0, cs, ROWS[0])
        if o == 1:
            return (y0, cs, b, ROWS[1])
        return (cs, b, z0, ROWS[2])

    def landed(o, b, cs):
        return (b, cs, ROWS[0]) if o == 0 else (cs, b, ROWS[o])

    def at2(o, k):
        return lax.rem(origin2[o] + k, 4)

    def at3(o, k):
        return lax.rem(origin3[o] + k, 4)

    groups = (
        ((LO, 0, 0), (HI, 1, 1)),
        ((LO, 0, 0), (HI, 1, 1)),
        tuple((at3(2, k), n % 2, n) for n, k in enumerate((2, 3, 1, 0))),
    )

    def take1(o, b, cs, lines=None):
        if o == 0:
            for kind in (PURE, ACC):
                for h in range(2):
                    wait1(kind, 0, (b, HALF[h]), 2 * b + h)
        elif o == 2:
            for kind in (PURE, ACC):
                wait1(kind, 2, (cs, b), 4 * cs + b)
        for c in range(4) if o < 2 else (cs,):
            p[held(o, b, c)] += ph1[(PURE,) + landed(o, b, c)] + ph1[(ACC,) + landed(o, b, c)]

    def all_of_order1():
        for kind in (PURE, ACC):
            for line in range(4):
                for h in range(2):
                    wait1(kind, 1, (line, HALF[h]), 2 * line + h)

    def copy2(kind, o, src, group, step):
        cs, _, n = group
        return remote(
            src, ph2.at[kind, cs, ROWS[o]], ss2.at[kind, o], rs2.at[kind, o, n], along2[o](step)
        )

    def wait2(kind, o, group):
        copy2(kind, o, ph2.at[kind, group[0], ROWS[o]], group, 1).wait_recv()

    def send2(kind, o, group, step):
        b = at2(o, 2 if kind == FAR else step)
        copy2(kind, o, p.at[held(o, b, group[0])], group, step).start()

    UP = (1, 3)
    DOWN = (3, 1)

    def accumulate2(o, group):
        cs, h, _ = group
        wait2(FAR, o, group)
        p[held(o, at2(o, UP[h]), cs)] += ph2[FAR, cs, ROWS[o]]
        send2(ACC, o, group, UP[h])

    def whole2(o):
        for group in groups[o]:
            send2(FAR, o, group, UP[group[1]])

    def pure2(o, step):
        for group in groups[o]:
            if DOWN[group[1]] == step:
                send2(PURE, o, group, step)

    def open2(n):
        group = groups[2][n]
        cs, h, _ = group
        take1(2, at2(2, 2), cs)
        send2(FAR, 2, group, UP[h])
        take1(2, at2(2, DOWN[h]), cs)
        send2(PURE, 2, group, DOWN[h])
        take1(2, at2(2, UP[h]), cs)

    def forwards(first, last):
        lax.fori_loop(first, last, lambda v, carry: (forward(v), carry)[1], 0)

    loads = [
        pltpu.make_async_copy(amp.at[k], s.at[pl.ds(DEPTH * k, DEPTH)], in_sem.at[k])
        for k in range(2)
    ]
    for load in loads:
        load.start()
    barrier = pltpu.get_barrier_semaphore()
    partners = [other_core] + [f(k) for f in along for k in (1, 3)]
    for device in partners:
        pl.semaphore_signal(barrier, inc=1, device_id=device, device_id_type=pl.DeviceIdType.MESH)
    for load in loads:
        load.wait()

    _, _, y, x = unit_of(0)
    for slot in range(2):
        transposed(slot, y)
    products(y, x)
    mend(y, x)
    pl.semaphore_wait(barrier, len(partners))
    core_copy(0, y, x).start()
    _, _, y, x = unit_of(1)
    products(y, x)
    mend(y, x)
    core_copy(1, y, x).start()

    def step(u, carry):
        _, _, y, x = unit_of(u)
        _, _, last_y, last_x = unit_of(u - 2)

        @pl.when(lax.rem(u, 4) == 0)
        def _():
            for slot in range(2):
                transposed(slot, y)
        core_copy(u - 2, last_y, last_x).wait_recv()
        products(y, x)
        add_cross(last_y, last_x)
        mend(y, x)
        core_copy(u, y, x).start()
        finish(u - 2)

        @pl.when(u >= 2 + LAG)
        def _():
            forward(u - 2 - LAG)

        @pl.when(u == 12)
        def _():
            take1(0, at2(0, 2), None)
            whole2(0)

        @pl.when(u == 13)
        def _():
            open2(0)

        return carry

    lax.fori_loop(2, 16, step, 0)
    def settle(v):
        _, _, y, x = unit_of(v)
        core_copy(v, y, x).wait_recv()
        add_cross(y, x)
        finish(v)

    settle(14)
    forward(11)
    take1(0, at2(0, 3), None)
    pure2(0, 3)
    accumulate2(2, groups[2][0])
    settle(15)
    forwards(12, 14)
    open2(1)
    forwards(14, 16)
    take1(0, at2(0, 1), None)
    pure2(0, 1)
    for group in groups[0]:
        accumulate2(0, group)
    all_of_order1()
    take1(1, at2(1, 2), None)
    whole2(1)
    for k in (3, 1):
        take1(1, at2(1, k), None)
        pure2(1, k)
    open2(2)
    accumulate2(2, groups[2][1])
    for group in groups[1]:
        accumulate2(1, group)
    open2(3)
    accumulate2(2, groups[2][2])
    accumulate2(2, groups[2][3])
    for o in range(2):
        take1(o, origin2[o], None)
    for c in range(4):
        take1(2, x0, c)

    def own(o, c):
        return held(o, origin2[o], c)

    def copy3(o, k, src):
        return remote(
            src, ph3.at[k - 1, ROWS[o]], ss3.at[k - 1, o], rs3.at[k - 1, o], along3[o](k)
        )

    def take2(o, c):
        p[own(o, c)] += ph2[PURE, c, ROWS[o]] + ph2[ACC, c, ROWS[o]]

    for o in (0, 2, 1):
        for group in groups[o]:
            for kind in (PURE, ACC):
                wait2(kind, o, group)
        for k in (2, 1, 3):
            c = at3(o, k)
            take2(o, c)
            copy3(o, k, p.at[own(o, c)]).start()
    for o in range(3):
        take2(o, origin3[o])

    row_block = 4 * core + y0
    col_block = 4 * x0 + z0
    xs, zs, phase = px[...], pz[...], pph[...]
    pick_row = lax.broadcasted_iota(jnp.int32, (128, TERMS), 0)
    pick = jnp.where(pick_row == (xs & 127), 1.0, 0.0).astype(jnp.bfloat16)
    term_row = 256 * row_block + lax.broadcasted_iota(jnp.int32, (256, TERMS), 0)
    sign = (1 - 2 * parity(term_row & zs)).astype(jnp.float32)
    weights[:, :TERMS] = jnp.where(((term_row >> 7) ^ (xs >> 7)) == col_block, sign, 0.0)
    even = (1 - parity(xs & zs)).astype(jnp.float32)
    scale = 1.0 / COLS
    real_weight = scale * jnp.where(xs == 0, 1.0, 2.0 * even)
    imag_weight = scale * (2.0 - 2.0 * even)
    phase_re = jnp.where(phase == 0, 1.0, jnp.where(phase == 2, -1.0, 0.0))
    phase_im = jnp.where(phase == 1, 1.0, jnp.where(phase == 3, -1.0, 0.0))

    for o in (0, 2, 1):
        for k in (1, 2, 3):
            copy3(o, k, ph3.at[k - 1, ROWS[o]]).wait_recv()
    block = p[y0, x0, z0] + ph3[0] + ph3[1] + ph3[2]
    p[y0, x0, z0] = block
    flipped[...] = block.T

    row = lax.broadcasted_iota(jnp.int32, (256, 128), 0)
    lane = lax.broadcasted_iota(jnp.int32, (256, 128), 1)
    moved = block
    for bit in range(7):
        hop = 1 << bit
        swapped = jnp.where(
            (lane & hop) != 0, pltpu.roll(moved, hop, 1), pltpu.roll(moved, 128 - hop, 1)
        )
        moved = jnp.where((row & hop) != 0, swapped, moved)
    in_row = 256 * row_block + row
    in_col = 128 * col_block + ((row & 127) ^ lane)
    high = moved.astype(jnp.bfloat16)
    rest = moved - high.astype(jnp.float32)
    middle = rest.astype(jnp.bfloat16)
    low = (rest - middle.astype(jnp.float32)).astype(jnp.bfloat16)
    upper = in_col >= in_row

    def read(keep):
        return sum(
            dot(jnp.where(keep, q.astype(jnp.float32), 0.0).astype(jnp.bfloat16), pick)
            for q in (high, middle, low)
        )

    weight = weights[:, :TERMS]
    sum_re = real_weight * jnp.sum(weight * read(upper), axis=0, keepdims=True)
    sum_im = imag_weight * jnp.sum(weight * read(~upper), axis=0, keepdims=True)
    here = jnp.concatenate(
        [phase_re * sum_re - phase_im * sum_im, phase_re * sum_im + phase_im * sum_re], axis=0
    )

    def give(here, parts, n, mine, count, where):
        parts[mine, :, :TERMS] = here
        for k in range(1, count):
            remote(
                parts.at[mine], parts.at[mine], ess.at[n], ers.at[n],
                where(lax.rem(mine + k, count)),
            ).start()

    def collect(parts, n, count):
        rest = parts.at[pl.ds(0, count - 1)]
        remote(rest, rest, ess.at[n], ers.at[n], other_core).wait_recv()
        total = parts[0, :, :TERMS]
        for k in range(1, count):
            total = total + parts[k, :, :TERMS]
        return total

    give(
        here, part0, 0, 4 * x0 + z0, 16,
        lambda k: {"gx": k // 4, "gy_0": lax.rem(k // 2, 2), "gz_1": lax.rem(k, 2)},
    )

    def device(e):
        return {
            "gx": e // 32,
            "gy_0": lax.rem(e // 16, 2),
            "gy_1": lax.rem(e // 8, 2),
            "gz_0": lax.rem(e // 2, 4),
            "gz_1": lax.rem(e, 2),
        }

    def direct_copy(k):
        e = 16 * row_block + k
        return e, remote(
            p.at[y0, x0, z0, pl.ds(16 * k, 16)], direct.at[col_block],
            dss.at[0], drs.at[0], device(e),
        )

    def mirror_copy(k):
        e = 8 * col_block + k
        return e, remote(
            flipped.at[pl.ds(16 * k, 16)], mirror.at[row_block],
            mss.at[0], mrs.at[0], device(e),
        )

    for k in range(16):
        e, copy = direct_copy(k)

        @pl.when(e != me)
        def _(copy=copy):
            copy.start()

        @pl.when(e == me)
        def _(k=k):
            direct[col_block] = p[y0, x0, z0, pl.ds(16 * k, 16)]

    for k in range(8):
        e, copy = mirror_copy(k)

        @pl.when(e != me)
        def _(copy=copy):
            copy.start()

        @pl.when(e == me)
        def _(k=k):
            mirror[row_block] = flipped[pl.ds(16 * k, 16)]

    give(
        collect(part0, 0, 16), part1, 1, 2 * y0 + core, 8,
        lambda k: {"gz_0": k // 2, "gy_1": lax.rem(k, 2)},
    )
    out_ex[...] = collect(part1, 1, 8)

    def landed_and_left(ref, ss, rs):
        copy = remote(ref, ref, ss, rs, other_core)
        copy.wait_recv()
        copy.wait_send()

    @pl.when(me // 16 == row_block)
    def _():
        landed_and_left(direct.at[pl.ds(0, 15)], dss.at[0], drs.at[0])

    @pl.when(me // 16 != row_block)
    def _():
        landed_and_left(direct, dss.at[0], drs.at[0])

    @pl.when(me // 8 == col_block)
    def _():
        landed_and_left(mirror.at[pl.ds(0, 7)], mss.at[0], mrs.at[0])

    @pl.when(me // 8 != col_block)
    def _():
        landed_and_left(mirror, mss.at[0], mrs.at[0])

    row = 16 * me + lax.broadcasted_iota(jnp.int32, (16, 128), 0)
    lane = lax.broadcasted_iota(jnp.int32, (16, 128), 1)
    for k in range(16):
        given = direct[k] * scale
        turned = mirror[k // 2, :, 128 * (k % 2) : 128 * (k % 2) + 128] * scale
        col = 128 * k + lane
        out_re[:, 128 * k : 128 * k + 128] = jnp.where(col >= row, given, turned)
        out_im[:, 128 * k : 128 * k + 128] = jnp.where(
            col < row, given, jnp.where(col == row, 0.0, -turned)
        )

    def left(ref, sem):
        remote(ref, ref, sem, core_rs.at[0], other_core).wait_send()

    left(stage, core_ss.at[0])
    for kind in range(3):
        for o in range(3):
            left(ph3.at[kind, ROWS[o]], ss3.at[kind, o])
            left(ph2.at[kind, :, ROWS[o]], ss2.at[kind, o])
            left(ph1.at[kind, :, :, ROWS[o]], ss1.at[kind, o])
    left(part0.at[pl.ds(0, 15)], ess.at[0])
    left(part1.at[pl.ds(0, 7)], ess.at[1])


def on_device(amplitudes, pauli_x, pauli_z, pauli_phase):
    vmem = pl.BlockSpec(memory_space=pltpu.VMEM)
    f32 = jnp.float32
    dma = pltpu.SemaphoreType.DMA
    return pl.pallas_call(
        kernel,
        out_shape=(
            jax.ShapeDtypeStruct((16, ORDER), f32),
            jax.ShapeDtypeStruct((16, ORDER), f32),
            jax.ShapeDtypeStruct((2, TERMS), f32),
        ),
        in_specs=[pl.BlockSpec(memory_space=pl.ANY), vmem, vmem, vmem],
        out_specs=(vmem, vmem, vmem),
        scratch_shapes=[
            pltpu.VMEM((2 * DEPTH, ORDER), jnp.bfloat16),
            pltpu.VMEM((2, 256, 3 * DEPTH), jnp.bfloat16),
            pltpu.VMEM((4, 4, 4, 256, 128), f32),
            pltpu.VMEM((4, 4, 4, 256, 128), f32),
            pltpu.VMEM((4, 4, 4, 256, 128), f32),
            pltpu.VMEM((3, 4, 4, 256, 128), f32),
            pltpu.VMEM((3, 4, 256, 128), f32),
            pltpu.VMEM((3, 256, 128), f32),
            pltpu.VMEM((128, 256), f32),
            pltpu.VMEM((16, 16, 128), f32),
            pltpu.VMEM((8, 16, 256), f32),
            pltpu.VMEM((256, TERMS_PAD), f32),
            pltpu.VMEM((16, 2, TERMS_PAD), f32),
            pltpu.VMEM((8, 2, TERMS_PAD), f32),
            dma((2,)),
            dma((1,)),
            dma((16,)),
            dma((3, 3)),
            dma((3, 32)),
            dma((3, 3)),
            dma((3, 3, 4)),
            dma((3, 3)),
            dma((3, 3)),
            dma((1,)),
            dma((1,)),
            dma((1,)),
            dma((1,)),
            dma((2,)),
            dma((2,)),
        ],
        compiler_params=pltpu.CompilerParams(
            collective_id=0, has_side_effects=True, vmem_limit_bytes=60 * 1024 * 1024
        ),
    )(amplitudes, pauli_x.reshape(1, TERMS), pauli_z.reshape(1, TERMS), pauli_phase.reshape(1, TERMS))


def solution(mesh):
    finer = Mesh(mesh.devices.reshape(mesh.shape["gx"], 2, 2, 4, 2), AXES)
    return jax.shard_map(
        on_device,
        mesh=finer,
        in_specs=(P(None, AXES, None), P(), P(), P()),
        out_specs=(P(AXES, None), P(AXES, None), P()),
        check_vma=False,
    )
```

```python
import functools

import jax
import jax.numpy as jnp
from jax import lax
from jax.experimental import pallas as pl
from jax.experimental.pallas import tpu as pltpu
from jax.sharding import Mesh
from jax.sharding import PartitionSpec as P

ORDER = 2048
COLS = 65536
DEPTH = 512
TERMS = 200
TERMS_PAD = 256
AXES = ("gx", "gy_0", "gy_1", "gz_0", "gz_1")
ROWS = (slice(0, 88), slice(88, 176), slice(176, 256))
FAR, PURE, ACC = 0, 1, 2
LAG_Z, LAG_XY = 3, 5
BASE = (0, 8, 16)
TAKE = (0, 4, 8)
UNITS = (
    (2, 2), (2, 3), (3, 2), (2, 1), (1, 2), (3, 3), (3, 1), (1, 3),
    (1, 1), (2, 0), (3, 0), (1, 0), (0, 2), (0, 3), (0, 1), (0, 0),
)
UNITS_Y = tuple(sum(u[0] << 2 * n for n, u in enumerate(UNITS[k : k + 8])) for k in (0, 8))
UNITS_X = tuple(sum(u[1] << 2 * n for n, u in enumerate(UNITS[k : k + 8])) for k in (0, 8))
LO, HI = slice(0, 2), slice(2, 4)
HALF = (LO, HI)


def digit(table, v):
    late = v // 8
    packed = table[0] + late * (table[1] - table[0])
    return (packed >> (2 * (v - 8 * late))) & 3


def remote(src, dst, send, recv, device):
    return pltpu.make_async_remote_copy(
        src_ref=src,
        dst_ref=dst,
        send_sem=send,
        recv_sem=recv,
        device_id=device,
        device_id_type=pl.DeviceIdType.MESH,
    )


def parity(values):
    values = values ^ (values >> 8)
    values = values ^ (values >> 4)
    values = values ^ (values >> 2)
    values = values ^ (values >> 1)
    return values & 1


def kernel(
    amp, px_in, pz_in, pph_in,
    out_re, out_im, out_ex,
    s, t, p, stage, cross, ph1, ph2, ph3, flipped, direct, mirror, weights, pick, part0, part1,
    px, pz, pph, in_sem, core_ss, core_rs, ss1, far1, take_s, ss2, far2, take2_s, ss3, rs3,
    dss, drs, mss, mrs, ess, ers,
):
    x0 = lax.axis_index("gx")
    zh = lax.axis_index("gy_0")
    core = lax.axis_index("gy_1")
    y0 = lax.axis_index("gz_0")
    zl = lax.axis_index("gz_1")
    z0 = 2 * zh + zl
    me = x0 * 32 + zh * 16 + core * 8 + y0 * 2 + zl

    def at_x(step):
        return {"gx": lax.rem(x0 + step, 4)}

    def at_y(step):
        return {"gz_0": lax.rem(y0 + step, 4)}

    def at_z(step):
        z = lax.rem(z0 + step, 4)
        return {"gy_0": z // 2, "gz_1": lax.rem(z, 2)}

    along = (at_x, at_y, at_z)
    along2 = (at_y, at_z, at_x)
    along3 = (at_z, at_x, at_y)
    origin2 = (y0, z0, x0)
    origin3 = (z0, x0, y0)
    other_core = {"gy_1": 1 - core}
    blocks = (4 * (1 - core), 4 * core)

    def transposed(slot, y):
        at = 2 * y + slot
        first = pl.multiple_of((blocks[slot] + y) * 256, 256)
        re_t = s[:DEPTH, pl.ds(first, 256)].T
        im_t = s[DEPTH:, pl.ds(first, 256)].T
        t[at, :, :DEPTH] = re_t
        t[at, :, DEPTH : 2 * DEPTH] = im_t
        t[at, :, 2 * DEPTH :] = -re_t

    def factor(slot, y, imag):
        return t[2 * y + slot, :, pl.ds(pl.multiple_of(imag * DEPTH, DEPTH), 2 * DEPTH)]

    def column(col):
        return s[:, pl.ds(pl.multiple_of(col * 256, 256), 256)]

    dot = functools.partial(jnp.dot, preferred_element_type=jnp.float32)

    def products(y, x):
        for half in range(2):
            col = 2 * x + half
            left = jnp.concatenate(
                [factor(slot, y, (blocks[slot] + y - col + 7) // 8) for slot in range(2)], axis=0
            )
            value = dot(left, column(col))
            for slot, dst in ((0, stage), (1, p)):
                for k in range(2):
                    dst[y, x, 2 * half + k] = value[
                        256 * slot : 256 * slot + 256, 128 * k : 128 * k + 128
                    ]

    def mend(y, x):
        for slot, dst in ((0, stage), (1, p)):
            block = blocks[slot] + y

            @pl.when(block // 2 == x)
            def _(slot=slot, dst=dst, block=block):
                imag = dot(factor(slot, y, 1), column(block))
                row = lax.broadcasted_iota(jnp.int32, (256, 128), 0)
                lane = lax.broadcasted_iota(jnp.int32, (256, 128), 1)
                for k in range(2):
                    z = 2 * lax.rem(block, 2) + k
                    dst[y, x, z] = jnp.where(
                        lane + 128 * k >= row, dst[y, x, z], imag[:, 128 * k : 128 * k + 128]
                    )

    def unit_of(v):
        off_y, off_x = digit(UNITS_Y, v), digit(UNITS_X, v)
        return off_y, off_x, lax.rem(y0 + off_y, 4), lax.rem(x0 + off_x, 4)

    def core_copy(v, y, x):
        return remote(stage.at[y, x], cross.at[y, x], core_ss.at[0], core_rs.at[v], other_core)

    def copy1(kind, o, src, key, index, step):
        line = index // 2 if o < 2 else index
        return remote(
            src,
            ph1.at[(kind,) + key + (ROWS[o],)],
            ss1.at[0],
            far1.at[BASE[o] + index] if kind == FAR else take_s.at[TAKE[o] + line],
            along[o](step),
        )

    def send1(kind, o, src, key, index, step):
        copy1(kind, o, src, key, index, step).start()

    def wait1(o, key, index):
        copy1(FAR, o, ph1.at[(FAR,) + key + (ROWS[o],)], key, index, 1).wait_recv()

    def add_cross(y, x):
        for z in range(4):
            p[y, x, z] += cross[y, x, z]

    def finish(v):
        off_y, off_x, y, x = unit_of(v)
        for o, off, line in ((0, off_x, y), (1, off_y, x)):
            @pl.when(off == 2)
            def _(o=o, line=line):
                for h, step in ((0, 1), (1, 3)):
                    send1(FAR, o, p.at[y, x, HALF[h], ROWS[o]], (line, HALF[h]), 2 * line + h, step)

            @pl.when(off == 1)
            def _(o=o, line=line):
                send1(PURE, o, p.at[y, x, HI, ROWS[o]], (line, HI), 2 * line + 1, 1)

            @pl.when(off == 3)
            def _(o=o, line=line):
                send1(PURE, o, p.at[y, x, LO, ROWS[o]], (line, LO), 2 * line, 3)

        up = lax.rem(v, 2)
        far, right, left = (lax.rem(z0 + k, 4) for k in (2, 1, 3))

        @pl.when(up == 0)
        def _():
            send1(FAR, 2, p.at[y, x, far, ROWS[2]], (y, x), 4 * y + x, 1)
            send1(PURE, 2, p.at[y, x, left, ROWS[2]], (y, x), 4 * y + x, 3)

        @pl.when(up == 1)
        def _():
            send1(FAR, 2, p.at[y, x, far, ROWS[2]], (y, x), 4 * y + x, 3)
            send1(PURE, 2, p.at[y, x, right, ROWS[2]], (y, x), 4 * y + x, 1)

    def forward_xy(v):
        off_y, off_x, y, x = unit_of(v)
        for o, off, line in ((0, off_x, y), (1, off_y, x)):
            for h, step in ((0, 1), (1, 3)):
                @pl.when(off == step)
                def _(o=o, line=line, h=h, step=step):
                    key, index = (line, HALF[h]), 2 * line + h
                    wait1(o, key, index)
                    p[y, x, HALF[h], ROWS[o]] += ph1[FAR, line, HALF[h], ROWS[o]]
                    send1(ACC, o, p.at[y, x, HALF[h], ROWS[o]], key, index, step)

    def forward_z(v):
        _, _, y, x = unit_of(v)
        wait1(2, (y, x), 4 * y + x)
        for h, step in ((0, 1), (1, 3)):
            @pl.when(lax.rem(v, 2) == h)
            def _(step=step):
                z = lax.rem(z0 + step, 4)
                p[y, x, z, ROWS[2]] += ph1[FAR, y, x, ROWS[2]]
                send1(ACC, 2, p.at[y, x, z, ROWS[2]], (y, x), 4 * y + x, step)

    def held(o, b, cs):
        if o == 0:
            return (b, x0, cs, ROWS[0])
        if o == 1:
            return (y0, cs, b, ROWS[1])
        return (cs, b, z0, ROWS[2])

    def landed(o, b, cs):
        return (b, cs, ROWS[0]) if o == 0 else (cs, b, ROWS[o])

    def at2(o, k):
        return lax.rem(origin2[o] + k, 4)

    def at3(o, k):
        return lax.rem(origin3[o] + k, 4)

    groups = ((((LO, 0, 0), (HI, 1, 1)),) + tuple(
        tuple((at3(o, k), n % 2, n) for n, k in enumerate((2, 3, 1, 0))) for o in (1, 2)
    ))

    def arrived(o, line):
        key = (line // 4, lax.rem(line, 4)) if o == 2 else (line, slice(None))
        ref = ph1.at[(slice(PURE, ACC + 1),) + key + (ROWS[o],)]
        remote(ref, ref, ss1.at[0], take_s.at[TAKE[o] + line], other_core).wait_recv()

    def add1(o, b, c):
        p[held(o, b, c)] += ph1[(PURE,) + landed(o, b, c)] + ph1[(ACC,) + landed(o, b, c)]

    def take0(b):
        arrived(0, b)
        for c in range(4):
            add1(0, b, c)

    def copy2(kind, o, src, group, step):
        cs, _, n = group
        return remote(
            src, ph2.at[kind, cs, ROWS[o]], ss2.at[0],
            far2.at[o, n] if kind == FAR else take2_s.at[o, n if o else 0], along2[o](step),
        )

    def wait2(o, group):
        copy2(FAR, o, ph2.at[FAR, group[0], ROWS[o]], group, 1).wait_recv()

    def send2(kind, o, group, step):
        b = at2(o, 2 if kind == FAR else step)
        copy2(kind, o, p.at[held(o, b, group[0])], group, step).start()

    UP = (1, 3)
    DOWN = (3, 1)

    def accumulate2(o, n):
        group = groups[o][n]
        cs, h, _ = group
        wait2(o, group)
        p[held(o, at2(o, UP[h]), cs)] += ph2[FAR, cs, ROWS[o]]
        send2(ACC, o, group, UP[h])

    def far0():
        take0(at2(0, 2))
        for group in groups[0]:
            send2(FAR, 0, group, UP[group[1]])

    def pure0(step):
        take0(at2(0, step))
        for group in groups[0]:
            if DOWN[group[1]] == step:
                send2(PURE, 0, group, step)

    def open2(o, n):
        group = groups[o][n]
        cs, h, _ = group

        def take(k):
            b = at2(o, k)
            if o == 2:
                arrived(2, 4 * cs + b)
            add1(o, b, cs)

        if o == 1:
            arrived(1, cs)
        take(2)
        send2(FAR, o, group, UP[h])
        take(DOWN[h])
        send2(PURE, o, group, DOWN[h])
        take(UP[h])

    def direct2(o):
        c = groups[o][3][0]
        if o == 1:
            arrived(1, c)
        for k in (2, 1, 3):
            b = at2(o, k)
            if o == 2:
                arrived(2, 4 * c + b)
            add1(o, b, c)
            remote(
                p.at[held(o, b, c)], ph2.at[k - 1, c, ROWS[o]],
                ss2.at[0], take2_s.at[o, 3], along2[o](k),
            ).start()

    def own(o, c):
        return held(o, origin2[o], c)

    def send3(o, k):
        remote(
            p.at[own(o, at3(o, k))], ph3.at[k - 1, ROWS[o]], ss3.at[0], rs3.at[o], along3[o](k)
        ).start()

    def close2(o, n):
        c = groups[o][n][0]
        if o == 2:
            arrived(2, 4 * c + x0)
        add1(o, origin2[o], c)
        ref = ph2.at[PURE : ACC + 1, c, ROWS[o]]
        remote(ref, ref, ss2.at[0], take2_s.at[o, n], other_core).wait_recv()
        p[own(o, c)] += ph2[PURE, c, ROWS[o]] + ph2[ACC, c, ROWS[o]]
        send3(o, (2, 3, 1)[n])

    def close0():
        take0(y0)
        ref = ph2.at[PURE : ACC + 1, :, ROWS[0]]
        remote(ref, ref, ss2.at[0], take2_s.at[0, 0], other_core).wait_recv()
        for k in (2, 1, 3, 0):
            c = at3(0, k)
            p[own(0, c)] += ph2[PURE, c, ROWS[0]] + ph2[ACC, c, ROWS[0]]
            if k:
                send3(0, k)

    loads = [
        pltpu.make_async_copy(amp.at[k], s.at[pl.ds(DEPTH * k, DEPTH)], in_sem.at[k])
        for k in range(2)
    ]
    for n, (src, dst) in enumerate(((px_in, px), (pz_in, pz), (pph_in, pph))):
        loads.append(pltpu.make_async_copy(src, dst, in_sem.at[2 + n]))
    for load in loads:
        load.start()
    barrier = pltpu.get_barrier_semaphore()
    partners = [other_core] + [f(k) for f in along for k in (1, 3)]
    for device in partners:
        pl.semaphore_signal(barrier, inc=1, device_id=device, device_id_type=pl.DeviceIdType.MESH)
    for load in loads:
        load.wait()

    for slot in range(2):
        transposed(slot, lax.rem(y0 + 2, 4))
    _, _, y, x = unit_of(0)
    products(y, x)
    mend(y, x)
    pl.semaphore_wait(barrier, len(partners))
    core_copy(0, y, x).start()
    _, _, y, x = unit_of(1)
    products(y, x)
    mend(y, x)
    core_copy(1, y, x).start()

    def settle(v):
        _, _, y, x = unit_of(v)
        core_copy(v, y, x).wait_recv()
        add_cross(y, x)
        finish(v)

    settle(0)
    _, _, y, x = unit_of(2)
    for slot in range(2):
        transposed(slot, y)
    products(y, x)
    mend(y, x)
    core_copy(2, y, x).start()

    def step(u, carry):
        off_y, off_x, y, x = unit_of(u)
        _, _, last_y, last_x = unit_of(u - 2)

        @pl.when(off_x == 2)
        def _():
            for slot in range(2):
                transposed(slot, y)
        core_copy(u - 2, last_y, last_x).wait_recv()
        products(y, x)
        add_cross(last_y, last_x)
        mend(y, x)
        core_copy(u, y, x).start()
        finish(u - 2)

        @pl.when(u >= 2 + LAG_Z)
        def _():
            forward_z(u - 2 - LAG_Z)

        @pl.when(u >= 2 + LAG_XY)
        def _():
            forward_xy(u - 2 - LAG_XY)

        @pl.when(u == 12)
        def _():
            open2(2, 0)

        return carry

    lax.fori_loop(3, 16, step, 0)

    settle(14)
    forward_z(11)
    forward_xy(10)
    accumulate2(2, 0)
    settle(15)
    forward_z(12)
    forward_z(13)
    forward_xy(11)
    far0()
    open2(1, 0)
    open2(2, 1)
    forward_z(14)
    forward_z(15)
    forward_xy(13)
    forward_xy(14)
    row_block = 4 * core + y0
    col_block = 4 * x0 + z0
    xs, zs, phase = px[...], pz[...], pph[...]
    even = parity(xs & zs) == 0
    for n in range(3):
        rows = slice(128 * n, 128 * n + 128)
        pick[rows, :TERMS] = jnp.where(
            lax.broadcasted_iota(jnp.int32, (128, TERMS), 0) == (xs & 127), 1.0, 0.0
        ).astype(jnp.bfloat16)
    count = jnp.where(xs == 0, 1.0, 2.0) * (1.0 / COLS)
    rows = 256 * row_block + lax.broadcasted_iota(jnp.int32, (256, TERMS), 0)
    sign = jnp.where(parity(rows & zs) == 0, count, -count)
    keep = ((rows ^ xs) >> 7) == col_block
    weights[:, :TERMS] = jnp.where(keep & (((rows ^ xs) >= rows) == even), sign, 0.0)

    def phased(share):
        phase_re = jnp.where(phase == 0, 1.0, jnp.where(phase == 2, -1.0, 0.0))
        phase_im = jnp.where(phase == 1, 1.0, jnp.where(phase == 3, -1.0, 0.0))
        return share * jnp.concatenate(
            [jnp.where(even, phase_re, -phase_im), jnp.where(even, phase_im, phase_re)], axis=0
        )
    pure0(3)
    open2(1, 1)
    pure0(1)
    open2(1, 2)
    open2(2, 2)
    accumulate2(1, 0)
    accumulate2(2, 1)
    for n in range(2):
        accumulate2(0, n)
    accumulate2(1, 1)
    direct2(1)
    close2(2, 0)
    accumulate2(1, 2)
    accumulate2(2, 2)
    close2(1, 0)
    close2(2, 1)
    close2(1, 1)
    direct2(2)
    close0()
    close2(1, 2)
    close2(2, 2)

    for o in (1, 2):
        c = origin3[o]
        if o == 2:
            arrived(2, 4 * c + x0)
        add1(o, origin2[o], c)
        ref = ph2.at[:, c, ROWS[o]]
        remote(ref, ref, ss2.at[0], take2_s.at[o, 3], other_core).wait_recv()
        p[own(o, c)] += ph2[0, c, ROWS[o]] + ph2[1, c, ROWS[o]] + ph2[2, c, ROWS[o]]
    for o in range(3):
        ref = ph3.at[:, ROWS[o]]
        remote(ref, ref, ss3.at[0], rs3.at[o], other_core).wait_recv()
    block = p[y0, x0, z0] + ph3[0] + ph3[1] + ph3[2]
    p[y0, x0, z0] = block

    row = lax.broadcasted_iota(jnp.int32, (256, 128), 0)
    lane = lax.broadcasted_iota(jnp.int32, (256, 128), 1)
    moved = block
    for bit in range(7):
        hop = 1 << bit
        swapped = jnp.where(
            (lane & hop) != 0, pltpu.roll(moved, hop, 1), pltpu.roll(moved, 128 - hop, 1)
        )
        moved = jnp.where((row & hop) != 0, swapped, moved)
    high = moved.astype(jnp.bfloat16)
    rest = moved - high.astype(jnp.float32)
    middle = rest.astype(jnp.bfloat16)
    low = (rest - middle.astype(jnp.float32)).astype(jnp.bfloat16)
    read = dot(jnp.concatenate([high, middle, low], axis=1), pick[:, :TERMS])
    here = jnp.sum(weights[:, :TERMS] * read, axis=0, keepdims=True)

    def give(here, parts, n, mine, count, where):
        parts[mine, :, :TERMS] = here
        for k in range(1, count):
            remote(
                parts.at[mine], parts.at[mine], ess.at[n], ers.at[n],
                where(lax.rem(mine + k, count)),
            ).start()

    def collect(parts, n, count):
        rest = parts.at[pl.ds(0, count - 1)]
        remote(rest, rest, ess.at[n], ers.at[n], other_core).wait_recv()
        total = parts[0, :, :TERMS]
        for k in range(1, count):
            total = total + parts[k, :, :TERMS]
        return total

    give(
        here, part0, 0, 4 * x0 + z0, 16,
        lambda k: {"gx": k // 4, "gy_0": lax.rem(k // 2, 2), "gz_1": lax.rem(k, 2)},
    )

    flipped[...] = block.T

    def device(e):
        return {
            "gx": e // 32,
            "gy_0": lax.rem(e // 16, 2),
            "gy_1": lax.rem(e // 8, 2),
            "gz_0": lax.rem(e // 2, 4),
            "gz_1": lax.rem(e, 2),
        }

    def direct_copy(k):
        e = 16 * row_block + k
        return e, remote(
            p.at[y0, x0, z0, pl.ds(16 * k, 16)], direct.at[col_block],
            dss.at[0], drs.at[0], device(e),
        )

    def mirror_copy(k):
        e = 8 * col_block + k
        return e, remote(
            flipped.at[pl.ds(16 * k, 16)], mirror.at[row_block],
            mss.at[0], mrs.at[0], device(e),
        )

    for k in range(16):
        e, copy = direct_copy(k)

        @pl.when(e != me)
        def _(copy=copy):
            copy.start()

        @pl.when(e == me)
        def _(k=k):
            direct[col_block] = p[y0, x0, z0, pl.ds(16 * k, 16)]

    for k in range(8):
        e, copy = mirror_copy(k)

        @pl.when(e != me)
        def _(copy=copy):
            copy.start()

        @pl.when(e == me)
        def _(k=k):
            mirror[row_block] = flipped[pl.ds(16 * k, 16)]

    give(
        collect(part0, 0, 16), part1, 1, 2 * y0 + core, 8,
        lambda k: {"gz_0": k // 2, "gy_1": lax.rem(k, 2)},
    )
    out_ex[...] = phased(collect(part1, 1, 8))

    def landed_and_left(ref, ss, rs):
        copy = remote(ref, ref, ss, rs, other_core)
        copy.wait_recv()
        copy.wait_send()

    @pl.when(me // 16 == row_block)
    def _():
        landed_and_left(direct.at[pl.ds(0, 15)], dss.at[0], drs.at[0])

    @pl.when(me // 16 != row_block)
    def _():
        landed_and_left(direct, dss.at[0], drs.at[0])

    @pl.when(me // 8 == col_block)
    def _():
        landed_and_left(mirror.at[pl.ds(0, 7)], mss.at[0], mrs.at[0])

    @pl.when(me // 8 != col_block)
    def _():
        landed_and_left(mirror, mss.at[0], mrs.at[0])

    row = 16 * me + lax.broadcasted_iota(jnp.int32, (16, 128), 0)
    lane = lax.broadcasted_iota(jnp.int32, (16, 128), 1)
    for k in range(16):
        given = direct[k] * (1.0 / COLS)
        turned = mirror[k // 2, :, 128 * (k % 2) : 128 * (k % 2) + 128] * (1.0 / COLS)
        col = 128 * k + lane
        out_re[:, 128 * k : 128 * k + 128] = jnp.where(col >= row, given, turned)
        out_im[:, 128 * k : 128 * k + 128] = jnp.where(
            col < row, given, jnp.where(col == row, 0.0, -turned)
        )

    def left(ref, sem):
        remote(ref, ref, sem, core_rs.at[0], other_core).wait_send()

    left(stage, core_ss.at[0])
    left(ph1, ss1.at[0])
    left(ph2, ss2.at[0])
    left(ph3, ss3.at[0])
    left(part0.at[pl.ds(0, 15)], ess.at[0])
    left(part1.at[pl.ds(0, 7)], ess.at[1])


def put_out(re, im, ex, out_re, out_im, out_ex):
    out_re[...] = re[...]
    out_im[...] = im[...]
    out_ex[...] = ex[...]


def on_device(amplitudes, pauli_x, pauli_z, pauli_phase):
    vmem = pl.BlockSpec(memory_space=pltpu.VMEM)
    f32 = jnp.float32
    dma = pltpu.SemaphoreType.DMA
    results = pl.pallas_call(
        kernel,
        out_shape=(
            jax.ShapeDtypeStruct((16, ORDER), f32),
            jax.ShapeDtypeStruct((16, ORDER), f32),
            jax.ShapeDtypeStruct((2, TERMS), f32),
        ),
        in_specs=[pl.BlockSpec(memory_space=pltpu.HBM)] * 4,
        out_specs=(vmem, vmem, vmem),
        scratch_shapes=[
            pltpu.VMEM((2 * DEPTH, ORDER), jnp.bfloat16),
            pltpu.VMEM((8, 256, 3 * DEPTH), jnp.bfloat16),
            pltpu.VMEM((4, 4, 4, 256, 128), f32),
            pltpu.VMEM((4, 4, 4, 256, 128), f32),
            pltpu.VMEM((4, 4, 4, 256, 128), f32),
            pltpu.VMEM((3, 4, 4, 256, 128), f32),
            pltpu.VMEM((3, 4, 256, 128), f32),
            pltpu.VMEM((3, 256, 128), f32),
            pltpu.VMEM((128, 256), f32),
            pltpu.VMEM((16, 16, 128), f32),
            pltpu.VMEM((8, 16, 256), f32),
            pltpu.VMEM((256, TERMS_PAD), f32),
            pltpu.VMEM((384, TERMS_PAD), jnp.bfloat16),
            pltpu.VMEM((16, 1, TERMS_PAD), f32),
            pltpu.VMEM((8, 1, TERMS_PAD), f32),
            pltpu.VMEM((1, TERMS), jnp.int32),
            pltpu.VMEM((1, TERMS), jnp.int32),
            pltpu.VMEM((1, TERMS), jnp.int32),
            dma((5,)),
            dma((1,)),
            dma((16,)),
            dma((1,)),
            dma((32,)),
            dma((24,)),
            dma((1,)),
            dma((3, 4)),
            dma((3, 4)),
            dma((1,)),
            dma((3,)),
            dma((1,)),
            dma((1,)),
            dma((1,)),
            dma((1,)),
            dma((2,)),
            dma((2,)),
        ],
        compiler_params=pltpu.CompilerParams(
            collective_id=0, has_side_effects=True, vmem_limit_bytes=45 * 1024 * 1024
        ),
    )(*(pltpu.with_memory_space_constraint(v, pltpu.HBM) for v in (amplitudes, pauli_x.reshape(1, TERMS), pauli_z.reshape(1, TERMS), pauli_phase.reshape(1, TERMS))))
    return pl.pallas_call(
        put_out,
        out_shape=tuple(jax.ShapeDtypeStruct(r.shape, f32) for r in results),
        in_specs=[vmem] * 3,
        out_specs=(vmem,) * 3,
        compiler_params=pltpu.CompilerParams(vmem_limit_bytes=4 * 1024 * 1024),
    )(*results)


def solution(mesh):
    finer = Mesh(mesh.devices.reshape(mesh.shape["gx"], 2, 2, 4, 2), AXES)
    return jax.shard_map(
        on_device,
        mesh=finer,
        in_specs=(P(None, AXES, None), P(), P(), P()),
        out_specs=(P(AXES, None), P(AXES, None), P()),
        check_vma=False,
    )
```

```python
import functools

import jax
import jax.numpy as jnp
from jax import lax
from jax.experimental import pallas as pl
from jax.experimental.pallas import tpu as pltpu
from jax.sharding import Mesh
from jax.sharding import PartitionSpec as P

ORDER = 2048
COLS = 65536
DEPTH = 512
TERMS = 200
TERMS_PAD = 256
AXES = ("gx", "gy_0", "gy_1", "gz_0", "gz_1")
ROWS = (slice(0, 88), slice(88, 176), slice(176, 256))
FAR, PURE, ACC = 0, 1, 2
LAG_Z, LAG_XY = 3, 3
BASE = (0, 8, 16)
TAKE = (0, 4, 8)
UNITS = (
    (2, 2), (2, 3), (3, 2), (2, 1), (1, 2), (3, 3), (3, 1), (1, 3),
    (1, 1), (2, 0), (3, 0), (1, 0), (0, 2), (0, 3), (0, 1), (0, 0),
)
UNITS_Y = tuple(sum(u[0] << 2 * n for n, u in enumerate(UNITS[k : k + 8])) for k in (0, 8))
UNITS_X = tuple(sum(u[1] << 2 * n for n, u in enumerate(UNITS[k : k + 8])) for k in (0, 8))
LO, HI = slice(0, 2), slice(2, 4)
HALF = (LO, HI)


def digit(table, v):
    late = v // 8
    packed = table[0] + late * (table[1] - table[0])
    return (packed >> (2 * (v - 8 * late))) & 3


def remote(src, dst, send, recv, device):
    return pltpu.make_async_remote_copy(
        src_ref=src,
        dst_ref=dst,
        send_sem=send,
        recv_sem=recv,
        device_id=device,
        device_id_type=pl.DeviceIdType.MESH,
    )


def parity(values):
    values = values ^ (values >> 8)
    values = values ^ (values >> 4)
    values = values ^ (values >> 2)
    values = values ^ (values >> 1)
    return values & 1


def kernel(
    amp, px_in, pz_in, pph_in,
    out_re, out_im, out_ex,
    s, t, p, stage, cross, ph1, ph2, ph3, flipped, direct, mirror, weights, pick, part0, part1,
    px, pz, pph, in_sem, core_ss, core_rs, ss1, far1, take_s, ss2, far2, take2_s, ss3, rs3,
    dss, drs, mss, mrs, ess, ers,
):
    x0 = lax.axis_index("gx")
    zh = lax.axis_index("gy_0")
    core = lax.axis_index("gy_1")
    y0 = lax.axis_index("gz_0")
    zl = lax.axis_index("gz_1")
    z0 = 2 * zh + zl
    me = x0 * 32 + zh * 16 + core * 8 + y0 * 2 + zl

    def at_x(step):
        return {"gx": lax.rem(x0 + step, 4)}

    def at_y(step):
        return {"gz_0": lax.rem(y0 + step, 4)}

    def at_z(step):
        z = lax.rem(z0 + step, 4)
        return {"gy_0": z // 2, "gz_1": lax.rem(z, 2)}

    along = (at_x, at_y, at_z)
    along2 = (at_y, at_z, at_x)
    along3 = (at_z, at_x, at_y)
    origin2 = (y0, z0, x0)
    origin3 = (z0, x0, y0)
    other_core = {"gy_1": 1 - core}
    blocks = (4 * (1 - core), 4 * core)

    def transposed(slot, y):
        at = 2 * y + slot
        first = pl.multiple_of((blocks[slot] + y) * 256, 256)
        re_t = s[:DEPTH, pl.ds(first, 256)].T
        im_t = s[DEPTH:, pl.ds(first, 256)].T
        t[at, :, :DEPTH] = re_t
        t[at, :, DEPTH : 2 * DEPTH] = im_t
        t[at, :, 2 * DEPTH :] = -re_t

    def factor(slot, y, imag):
        return t[2 * y + slot, :, pl.ds(pl.multiple_of(imag * DEPTH, DEPTH), 2 * DEPTH)]

    def column(col):
        return s[:, pl.ds(pl.multiple_of(col * 256, 256), 256)]

    dot = functools.partial(jnp.dot, preferred_element_type=jnp.float32)

    def half_product(slot, dst, y, x, half):
        block, col = blocks[slot] + y, 2 * x + half
        value = dot(factor(slot, y, (block - col + 7) // 8), column(col))
        for k in range(2):
            dst[y, x, 2 * half + k] = value[:, 128 * k : 128 * k + 128]

    def products(y, x):
        for half in range(2):
            col = 2 * x + half
            left = jnp.concatenate(
                [factor(slot, y, (blocks[slot] + y - col + 7) // 8) for slot in range(2)], axis=0
            )
            value = dot(left, column(col))
            for slot, dst in ((0, stage), (1, p)):
                for k in range(2):
                    dst[y, x, 2 * half + k] = value[
                        256 * slot : 256 * slot + 256, 128 * k : 128 * k + 128
                    ]

    def mend(y, x, slots=(0, 1)):
        for slot in slots:
            dst = p if slot else stage
            block = blocks[slot] + y

            @pl.when(block // 2 == x)
            def _(slot=slot, dst=dst, block=block):
                imag = dot(factor(slot, y, 1), column(block))
                row = lax.broadcasted_iota(jnp.int32, (256, 128), 0)
                lane = lax.broadcasted_iota(jnp.int32, (256, 128), 1)
                for k in range(2):
                    z = 2 * lax.rem(block, 2) + k
                    dst[y, x, z] = jnp.where(
                        lane + 128 * k >= row, dst[y, x, z], imag[:, 128 * k : 128 * k + 128]
                    )

    def unit_of(v):
        off_y, off_x = digit(UNITS_Y, v), digit(UNITS_X, v)
        return off_y, off_x, lax.rem(y0 + off_y, 4), lax.rem(x0 + off_x, 4)

    def core_copy(v, y, x):
        return remote(stage.at[y, x], cross.at[y, x], core_ss.at[0], core_rs.at[v], other_core)

    def core_half(y, x, half):
        return remote(
            stage.at[y, x, HALF[half]], cross.at[y, x, HALF[half]],
            core_ss.at[0], core_rs.at[16 * half], other_core,
        )

    def copy1(kind, o, src, key, index, step):
        line = index // 2 if o < 2 else index
        return remote(
            src,
            ph1.at[(kind,) + key + (ROWS[o],)],
            ss1.at[0],
            far1.at[BASE[o] + index] if kind == FAR else take_s.at[TAKE[o] + line],
            along[o](step),
        )

    def send1(kind, o, src, key, index, step):
        copy1(kind, o, src, key, index, step).start()

    def wait1(o, key, index):
        copy1(FAR, o, ph1.at[(FAR,) + key + (ROWS[o],)], key, index, 1).wait_recv()

    def add_cross(y, x):
        for z in range(4):
            p[y, x, z] += cross[y, x, z]

    def finish(v):
        off_y, off_x, y, x = unit_of(v)
        for o, off, line in ((0, off_x, y), (1, off_y, x)):
            @pl.when(off == 2)
            def _(o=o, line=line):
                for h, step in ((0, 1), (1, 3)):
                    send1(FAR, o, p.at[y, x, HALF[h], ROWS[o]], (line, HALF[h]), 2 * line + h, step)

            @pl.when(off == 1)
            def _(o=o, line=line):
                send1(PURE, o, p.at[y, x, HI, ROWS[o]], (line, HI), 2 * line + 1, 1)

            @pl.when(off == 3)
            def _(o=o, line=line):
                send1(PURE, o, p.at[y, x, LO, ROWS[o]], (line, LO), 2 * line, 3)

        up = lax.rem(v, 2)
        far, right, left = (lax.rem(z0 + k, 4) for k in (2, 1, 3))

        @pl.when(up == 0)
        def _():
            send1(FAR, 2, p.at[y, x, far, ROWS[2]], (y, x), 4 * y + x, 1)
            send1(PURE, 2, p.at[y, x, left, ROWS[2]], (y, x), 4 * y + x, 3)

        @pl.when(up == 1)
        def _():
            send1(FAR, 2, p.at[y, x, far, ROWS[2]], (y, x), 4 * y + x, 3)
            send1(PURE, 2, p.at[y, x, right, ROWS[2]], (y, x), 4 * y + x, 1)

    def forward_xy(v):
        off_y, off_x, y, x = unit_of(v)
        for o, off, line in ((0, off_x, y), (1, off_y, x)):
            for h, step in ((0, 1), (1, 3)):
                @pl.when(off == step)
                def _(o=o, line=line, h=h, step=step):
                    key, index = (line, HALF[h]), 2 * line + h
                    wait1(o, key, index)
                    p[y, x, HALF[h], ROWS[o]] += ph1[FAR, line, HALF[h], ROWS[o]]
                    send1(ACC, o, p.at[y, x, HALF[h], ROWS[o]], key, index, step)

    def forward_z(v):
        _, _, y, x = unit_of(v)
        wait1(2, (y, x), 4 * y + x)
        for h, step in ((0, 1), (1, 3)):
            @pl.when(lax.rem(v, 2) == h)
            def _(step=step):
                z = lax.rem(z0 + step, 4)
                p[y, x, z, ROWS[2]] += ph1[FAR, y, x, ROWS[2]]
                send1(ACC, 2, p.at[y, x, z, ROWS[2]], (y, x), 4 * y + x, step)

    def held(o, b, cs):
        if o == 0:
            return (b, x0, cs, ROWS[0])
        if o == 1:
            return (y0, cs, b, ROWS[1])
        return (cs, b, z0, ROWS[2])

    def landed(o, b, cs):
        return (b, cs, ROWS[0]) if o == 0 else (cs, b, ROWS[o])

    def at2(o, k):
        return lax.rem(origin2[o] + k, 4)

    def at3(o, k):
        return lax.rem(origin3[o] + k, 4)

    groups = ((((LO, 0, 0), (HI, 1, 1)),) + tuple(
        tuple((at3(o, k), n % 2, n) for n, k in enumerate((2, 3, 1, 0))) for o in (1, 2)
    ))

    def arrived(o, line):
        key = (line // 4, lax.rem(line, 4)) if o == 2 else (line, slice(None))
        ref = ph1.at[(slice(PURE, ACC + 1),) + key + (ROWS[o],)]
        remote(ref, ref, ss1.at[0], take_s.at[TAKE[o] + line], other_core).wait_recv()

    def add1(o, b, c):
        p[held(o, b, c)] += ph1[(PURE,) + landed(o, b, c)] + ph1[(ACC,) + landed(o, b, c)]

    def take0(b):
        arrived(0, b)
        for c in range(4):
            add1(0, b, c)

    def copy2(kind, o, src, group, step):
        cs, _, n = group
        return remote(
            src, ph2.at[kind, cs, ROWS[o]], ss2.at[0],
            far2.at[o, n] if kind == FAR else take2_s.at[o, n if o else 0], along2[o](step),
        )

    def wait2(o, group):
        copy2(FAR, o, ph2.at[FAR, group[0], ROWS[o]], group, 1).wait_recv()

    def send2(kind, o, group, step):
        b = at2(o, 2 if kind == FAR else step)
        copy2(kind, o, p.at[held(o, b, group[0])], group, step).start()

    UP = (1, 3)
    DOWN = (3, 1)

    def accumulate2(o, n):
        group = groups[o][n]
        cs, h, _ = group
        wait2(o, group)
        p[held(o, at2(o, UP[h]), cs)] += ph2[FAR, cs, ROWS[o]]
        send2(ACC, o, group, UP[h])

    def far0():
        take0(at2(0, 2))
        for group in groups[0]:
            send2(FAR, 0, group, UP[group[1]])

    def pure0(step):
        take0(at2(0, step))
        for group in groups[0]:
            if DOWN[group[1]] == step:
                send2(PURE, 0, group, step)

    def open2(o, n):
        group = groups[o][n]
        cs, h, _ = group

        def take(k):
            b = at2(o, k)
            if o == 2:
                arrived(2, 4 * cs + b)
            add1(o, b, cs)

        if o == 1:
            arrived(1, cs)
        take(2)
        send2(FAR, o, group, UP[h])
        take(DOWN[h])
        send2(PURE, o, group, DOWN[h])
        take(UP[h])

    def direct2(o):
        c = groups[o][3][0]
        if o == 1:
            arrived(1, c)
        for k in (2, 1, 3):
            b = at2(o, k)
            if o == 2:
                arrived(2, 4 * c + b)
            add1(o, b, c)
            remote(
                p.at[held(o, b, c)], ph2.at[k - 1, c, ROWS[o]],
                ss2.at[0], take2_s.at[o, 3], along2[o](k),
            ).start()

    def own(o, c):
        return held(o, origin2[o], c)

    def send3(o, k):
        remote(
            p.at[own(o, at3(o, k))], ph3.at[k - 1, ROWS[o]], ss3.at[0], rs3.at[o], along3[o](k)
        ).start()

    def close2(o, n):
        c = groups[o][n][0]
        if o == 2:
            arrived(2, 4 * c + x0)
        add1(o, origin2[o], c)
        ref = ph2.at[PURE : ACC + 1, c, ROWS[o]]
        remote(ref, ref, ss2.at[0], take2_s.at[o, n], other_core).wait_recv()
        p[own(o, c)] += ph2[PURE, c, ROWS[o]] + ph2[ACC, c, ROWS[o]]
        send3(o, (2, 3, 1)[n])

    def close0():
        take0(y0)
        ref = ph2.at[PURE : ACC + 1, :, ROWS[0]]
        remote(ref, ref, ss2.at[0], take2_s.at[0, 0], other_core).wait_recv()
        for k in (2, 1, 3, 0):
            c = at3(0, k)
            p[own(0, c)] += ph2[PURE, c, ROWS[0]] + ph2[ACC, c, ROWS[0]]
            if k:
                send3(0, k)

    loads = [
        pltpu.make_async_copy(amp.at[k], s.at[pl.ds(DEPTH * k, DEPTH)], in_sem.at[k])
        for k in range(2)
    ]
    for n, (src, dst) in enumerate(((px_in, px), (pz_in, pz), (pph_in, pph))):
        loads.append(pltpu.make_async_copy(src, dst, in_sem.at[2 + n]))
    for load in loads:
        load.start()
    barrier = pltpu.get_barrier_semaphore()
    partners = [other_core] + [f(k) for f in along for k in (1, 3)]
    for device in partners:
        pl.semaphore_signal(barrier, inc=1, device_id=device, device_id_type=pl.DeviceIdType.MESH)
    for load in loads:
        load.wait()

    _, _, y, x = unit_of(0)
    transposed(0, y)
    half_product(0, stage, y, x, 0)
    half_product(0, stage, y, x, 1)
    mend(y, x, (0,))
    pl.semaphore_wait(barrier, len(partners))
    for half in range(2):
        core_half(y, x, half).start()
    transposed(1, y)
    half_product(1, p, y, x, 0)
    half_product(1, p, y, x, 1)
    mend(y, x, (1,))
    _, _, next_y, next_x = unit_of(1)
    products(next_y, next_x)
    mend(next_y, next_x)
    core_copy(1, next_y, next_x).start()

    def settle(v):
        _, _, y, x = unit_of(v)
        core_copy(v, y, x).wait_recv()
        add_cross(y, x)
        finish(v)

    for half in range(2):
        core_half(y, x, half).wait_recv()
    for z in range(4):
        p[y, x, z] += cross[y, x, z]
    finish(0)
    _, _, y, x = unit_of(2)
    for slot in range(2):
        transposed(slot, y)
    products(y, x)
    mend(y, x)
    core_copy(2, y, x).start()

    def step(u, carry):
        off_y, off_x, y, x = unit_of(u)
        _, _, last_y, last_x = unit_of(u - 2)

        @pl.when(off_x == 2)
        def _():
            for slot in range(2):
                transposed(slot, y)
        core_copy(u - 2, last_y, last_x).wait_recv()
        products(y, x)
        add_cross(last_y, last_x)
        mend(y, x)
        core_copy(u, y, x).start()
        finish(u - 2)

        @pl.when(u >= 2 + LAG_Z)
        def _():
            forward_z(u - 2 - LAG_Z)

        @pl.when(u >= 2 + LAG_XY)
        def _():
            forward_xy(u - 2 - LAG_XY)

        @pl.when(u == 12)
        def _():
            open2(2, 0)

        @pl.when(u == 13)
        def _():
            far0()

        @pl.when(u == 15)
        def _():
            open2(1, 0)
            open2(2, 1)

        return carry

    lax.fori_loop(3, 16, step, 0)

    settle(14)
    forward_z(11)
    pure0(3)
    settle(15)
    forward_z(12)
    forward_xy(11)
    forward_z(13)
    forward_xy(13)
    accumulate2(2, 0)
    open2(1, 1)
    forward_z(14)
    forward_xy(14)
    forward_z(15)
    row_block = 4 * core + y0
    col_block = 4 * x0 + z0
    xs, zs, phase = px[...], pz[...], pph[...]
    even = parity(xs & zs) == 0
    for n in range(3):
        rows = slice(128 * n, 128 * n + 128)
        pick[rows, :TERMS] = jnp.where(
            lax.broadcasted_iota(jnp.int32, (128, TERMS), 0) == (xs & 127), 1.0, 0.0
        ).astype(jnp.bfloat16)
    count = jnp.where(xs == 0, 1.0, 2.0) * (1.0 / COLS)
    row = lax.broadcasted_iota(jnp.int32, (256, TERMS), 0)
    for c in range(4):
        cols = jnp.where(row < 88, 4 * x0 + c, jnp.where(row < 176, 4 * c + z0, col_block))
        rows = 256 * jnp.where(row < 176, row_block, 4 * core + c) + row
        sign = jnp.where(parity(rows & zs) == 0, count, -count)
        keep = ((rows ^ xs) >> 7) == cols
        weights[256 * c : 256 * c + 256, :TERMS] = jnp.where(
            keep & (((rows ^ xs) >= rows) == even), sign, 0.0
        )

    def phased(share):
        phase_re = jnp.where(phase == 0, 1.0, jnp.where(phase == 2, -1.0, 0.0))
        phase_im = jnp.where(phase == 1, 1.0, jnp.where(phase == 3, -1.0, 0.0))
        return share * jnp.concatenate(
            [jnp.where(even, phase_re, -phase_im), jnp.where(even, phase_im, phase_re)], axis=0
        )
    pure0(1)
    open2(2, 2)
    open2(1, 2)
    accumulate2(1, 0)
    accumulate2(2, 1)
    accumulate2(0, 1)
    accumulate2(0, 0)
    accumulate2(1, 1)
    close2(2, 0)
    direct2(2)
    direct2(1)
    close2(1, 0)
    accumulate2(2, 2)
    accumulate2(1, 2)
    close2(2, 1)
    close2(1, 1)
    close0()
    close2(2, 2)
    close2(1, 2)

    for o in (1, 2):
        c = origin3[o]
        if o == 2:
            arrived(2, 4 * c + x0)
        add1(o, origin2[o], c)
        ref = ph2.at[:, c, ROWS[o]]
        remote(ref, ref, ss2.at[0], take2_s.at[o, 3], other_core).wait_recv()
        p[own(o, c)] += ph2[0, c, ROWS[o]] + ph2[1, c, ROWS[o]] + ph2[2, c, ROWS[o]]

    moved = jnp.concatenate([p[own(o, c)] for c in range(4) for o in range(3)], axis=0)
    row = lax.broadcasted_iota(jnp.int32, (1024, 128), 0)
    lane = lax.broadcasted_iota(jnp.int32, (1024, 128), 1)
    for bit in range(7):
        hop = 1 << bit
        if bit < 3:
            swapped = jnp.where(
                (lane & hop) != 0, pltpu.roll(moved, hop, 1), pltpu.roll(moved, 128 - hop, 1)
            )
            moved = jnp.where((row & hop) != 0, swapped, moved)
        else:
            runs = []
            for first in range(0, 1024, 2 * hop):
                runs.append(moved[first : first + hop])
                run = moved[first + hop : first + 2 * hop]
                if bit < 6:
                    run = jnp.where(
                        (lane[:hop] & hop) != 0,
                        pltpu.roll(run, hop, 1), pltpu.roll(run, 128 - hop, 1),
                    )
                else:
                    run = pltpu.roll(run, hop, 1)
                runs.append(run)
            moved = jnp.concatenate(runs, axis=0)
    high = moved.astype(jnp.bfloat16)
    rest = moved - high.astype(jnp.float32)
    middle = rest.astype(jnp.bfloat16)
    low = (rest - middle.astype(jnp.float32)).astype(jnp.bfloat16)
    read = dot(jnp.concatenate([high, middle, low], axis=1), pick[:, :TERMS])
    here = jnp.sum(weights[:, :TERMS] * read, axis=0, keepdims=True)

    def give(here, parts, n, mine, count, where):
        parts[mine, :, :TERMS] = here
        for k in range(1, count):
            remote(
                parts.at[mine], parts.at[mine], ess.at[n], ers.at[n],
                where(lax.rem(mine + k, count)),
            ).start()

    def collect(parts, n, count):
        rest = parts.at[pl.ds(0, count - 1)]
        remote(rest, rest, ess.at[n], ers.at[n], other_core).wait_recv()
        total = parts[0, :, :TERMS]
        for k in range(1, count):
            total = total + parts[k, :, :TERMS]
        return total

    give(
        here, part0, 0, 4 * x0 + z0, 16,
        lambda k: {"gx": k // 4, "gy_0": lax.rem(k // 2, 2), "gz_1": lax.rem(k, 2)},
    )

    for o in range(3):
        ref = ph3.at[:, ROWS[o]]
        remote(ref, ref, ss3.at[0], rs3.at[o], other_core).wait_recv()
    block = p[y0, x0, z0] + ph3[0] + ph3[1] + ph3[2]
    p[y0, x0, z0] = block

    flipped[...] = block.T

    def device(e):
        return {
            "gx": e // 32,
            "gy_0": lax.rem(e // 16, 2),
            "gy_1": lax.rem(e // 8, 2),
            "gz_0": lax.rem(e // 2, 4),
            "gz_1": lax.rem(e, 2),
        }

    def direct_copy(k):
        e = 16 * row_block + k
        return e, remote(
            p.at[y0, x0, z0, pl.ds(16 * k, 16)], direct.at[col_block],
            dss.at[0], drs.at[0], device(e),
        )

    def mirror_copy(k):
        e = 8 * col_block + k
        return e, remote(
            flipped.at[pl.ds(16 * k, 16)], mirror.at[row_block],
            mss.at[0], mrs.at[0], device(e),
        )

    @pl.when(me // 16 != row_block)
    def _():
        for k in range(16):
            direct_copy(k)[1].start()

    @pl.when(me // 16 == row_block)
    def _():
        for k in range(16):
            e, copy = direct_copy(k)
            pl.when(e != me)(copy.start)

            @pl.when(e == me)
            def _(k=k):
                direct[col_block] = p[y0, x0, z0, pl.ds(16 * k, 16)]

    @pl.when(me // 8 != col_block)
    def _():
        for k in range(8):
            mirror_copy(k)[1].start()

    @pl.when(me // 8 == col_block)
    def _():
        for k in range(8):
            e, copy = mirror_copy(k)
            pl.when(e != me)(copy.start)

            @pl.when(e == me)
            def _(k=k):
                mirror[row_block] = flipped[pl.ds(16 * k, 16)]

    give(
        collect(part0, 0, 16), part1, 1, 2 * y0 + core, 8,
        lambda k: {"gz_0": k // 2, "gy_1": lax.rem(k, 2)},
    )
    out_ex[...] = phased(collect(part1, 1, 8))

    def landed_and_left(ref, ss, rs):
        copy = remote(ref, ref, ss, rs, other_core)
        copy.wait_recv()
        copy.wait_send()

    @pl.when(me // 16 == row_block)
    def _():
        landed_and_left(direct.at[pl.ds(0, 15)], dss.at[0], drs.at[0])

    @pl.when(me // 16 != row_block)
    def _():
        landed_and_left(direct, dss.at[0], drs.at[0])

    @pl.when(me // 8 == col_block)
    def _():
        landed_and_left(mirror.at[pl.ds(0, 7)], mss.at[0], mrs.at[0])

    @pl.when(me // 8 != col_block)
    def _():
        landed_and_left(mirror, mss.at[0], mrs.at[0])

    row = 16 * me + lax.broadcasted_iota(jnp.int32, (16, 128), 0)
    lane = lax.broadcasted_iota(jnp.int32, (16, 128), 1)
    for k in range(16):
        given = direct[k] * (1.0 / COLS)
        turned = mirror[k // 2, :, 128 * (k % 2) : 128 * (k % 2) + 128] * (1.0 / COLS)
        col = 128 * k + lane
        out_re[:, 128 * k : 128 * k + 128] = jnp.where(col >= row, given, turned)
        out_im[:, 128 * k : 128 * k + 128] = jnp.where(
            col < row, given, jnp.where(col == row, 0.0, -turned)
        )

    def left(ref, sem):
        remote(ref, ref, sem, core_rs.at[0], other_core).wait_send()

    left(stage, core_ss.at[0])
    left(ph1, ss1.at[0])
    left(ph2, ss2.at[0])
    left(ph3, ss3.at[0])
    left(part0.at[pl.ds(0, 15)], ess.at[0])
    left(part1.at[pl.ds(0, 7)], ess.at[1])


def put_out(re, im, ex, out_re, out_im, out_ex):
    out_re[...] = re[...]
    out_im[...] = im[...]
    out_ex[...] = ex[...]


def on_device(amplitudes, pauli_x, pauli_z, pauli_phase):
    vmem = pl.BlockSpec(memory_space=pltpu.VMEM)
    f32 = jnp.float32
    dma = pltpu.SemaphoreType.DMA
    results = pl.pallas_call(
        kernel,
        out_shape=(
            jax.ShapeDtypeStruct((16, ORDER), f32),
            jax.ShapeDtypeStruct((16, ORDER), f32),
            jax.ShapeDtypeStruct((2, TERMS), f32),
        ),
        in_specs=[pl.BlockSpec(memory_space=pltpu.HBM)] * 4,
        out_specs=(vmem, vmem, vmem),
        scratch_shapes=[
            pltpu.VMEM((2 * DEPTH, ORDER), jnp.bfloat16),
            pltpu.VMEM((8, 256, 3 * DEPTH), jnp.bfloat16),
            pltpu.VMEM((4, 4, 4, 256, 128), f32),
            pltpu.VMEM((4, 4, 4, 256, 128), f32),
            pltpu.VMEM((4, 4, 4, 256, 128), f32),
            pltpu.VMEM((3, 4, 4, 256, 128), f32),
            pltpu.VMEM((3, 4, 256, 128), f32),
            pltpu.VMEM((3, 256, 128), f32),
            pltpu.VMEM((128, 256), f32),
            pltpu.VMEM((16, 16, 128), f32),
            pltpu.VMEM((8, 16, 256), f32),
            pltpu.VMEM((1024, TERMS_PAD), f32),
            pltpu.VMEM((384, TERMS_PAD), jnp.bfloat16),
            pltpu.VMEM((16, 1, TERMS_PAD), f32),
            pltpu.VMEM((8, 1, TERMS_PAD), f32),
            pltpu.VMEM((1, TERMS), jnp.int32),
            pltpu.VMEM((1, TERMS), jnp.int32),
            pltpu.VMEM((1, TERMS), jnp.int32),
            dma((5,)),
            dma((1,)),
            dma((17,)),
            dma((1,)),
            dma((32,)),
            dma((24,)),
            dma((1,)),
            dma((3, 4)),
            dma((3, 4)),
            dma((1,)),
            dma((3,)),
            dma((1,)),
            dma((1,)),
            dma((1,)),
            dma((1,)),
            dma((2,)),
            dma((2,)),
        ],
        compiler_params=pltpu.CompilerParams(
            collective_id=0, has_side_effects=True, vmem_limit_bytes=50 * 1024 * 1024
        ),
    )(*(pltpu.with_memory_space_constraint(v, pltpu.HBM) for v in (amplitudes, pauli_x.reshape(1, TERMS), pauli_z.reshape(1, TERMS), pauli_phase.reshape(1, TERMS))))
    return pl.pallas_call(
        put_out,
        out_shape=tuple(jax.ShapeDtypeStruct(r.shape, f32) for r in results),
        in_specs=[vmem] * 3,
        out_specs=(vmem,) * 3,
        compiler_params=pltpu.CompilerParams(vmem_limit_bytes=4 * 1024 * 1024),
    )(*results)


def solution(mesh):
    finer = Mesh(mesh.devices.reshape(mesh.shape["gx"], 2, 2, 4, 2), AXES)
    return jax.shard_map(
        on_device,
        mesh=finer,
        in_specs=(P(None, AXES, None), P(), P(), P()),
        out_specs=(P(AXES, None), P(AXES, None), P()),
        check_vma=False,
    )
```

```python
import functools

import jax
import jax.numpy as jnp
from jax import lax
from jax.experimental import pallas as pl
from jax.experimental.pallas import tpu as pltpu
from jax.sharding import Mesh
from jax.sharding import PartitionSpec as P

ORDER = 2048
COLS = 65536
DEPTH = 512
TERMS = 200
TERMS_PAD = 256
AXES = ("gx", "gy_0", "gy_1", "gz_0", "gz_1")
ROWS = (slice(0, 88), slice(88, 176), slice(176, 256))
FAR, PURE, ACC = 0, 1, 2
LAG_Z, LAG_XY = 3, 3
BASE = (0, 8, 16)
TAKE = (0, 4, 8)
UNITS = (
    (2, 2), (2, 3), (3, 2), (2, 1), (1, 2), (3, 3), (3, 1), (1, 3),
    (1, 1), (2, 0), (3, 0), (1, 0), (0, 2), (0, 3), (0, 1), (0, 0),
)
UNITS_Y = tuple(sum(u[0] << 2 * n for n, u in enumerate(UNITS[k : k + 8])) for k in (0, 8))
UNITS_X = tuple(sum(u[1] << 2 * n for n, u in enumerate(UNITS[k : k + 8])) for k in (0, 8))
LO, HI = slice(0, 2), slice(2, 4)
HALF = (LO, HI)


def digit(table, v):
    late = v // 8
    packed = table[0] + late * (table[1] - table[0])
    return (packed >> (2 * (v - 8 * late))) & 3


def remote(src, dst, send, recv, device):
    return pltpu.make_async_remote_copy(
        src_ref=src,
        dst_ref=dst,
        send_sem=send,
        recv_sem=recv,
        device_id=device,
        device_id_type=pl.DeviceIdType.MESH,
    )


def parity(values):
    values = values ^ (values >> 8)
    values = values ^ (values >> 4)
    values = values ^ (values >> 2)
    values = values ^ (values >> 1)
    return values & 1


def kernel(
    amp, px_in, pz_in, pph_in,
    out_re, out_im, out_ex,
    s, t, lower, p, stage, cross, ph1, ph2, ph3, flipped, direct, mirror, weights, pick, shares, part0, part1,
    px, pz, pph, in_sem, core_ss, core_rs, ss1, far1, take_s, ss2, far2, take2_s, ss3, rs3,
    dss, drs, mss, mrs, ess, ers,
):
    x0 = lax.axis_index("gx")
    zh = lax.axis_index("gy_0")
    core = lax.axis_index("gy_1")
    y0 = lax.axis_index("gz_0")
    zl = lax.axis_index("gz_1")
    z0 = 2 * zh + zl
    me = x0 * 32 + zh * 16 + core * 8 + y0 * 2 + zl

    def at_x(step):
        return {"gx": lax.rem(x0 + step, 4)}

    def at_y(step):
        return {"gz_0": lax.rem(y0 + step, 4)}

    def at_z(step):
        z = lax.rem(z0 + step, 4)
        return {"gy_0": z // 2, "gz_1": lax.rem(z, 2)}

    along = (at_x, at_y, at_z)
    along2 = (at_y, at_z, at_x)
    along3 = (at_z, at_x, at_y)
    origin2 = (y0, z0, x0)
    origin3 = (z0, x0, y0)
    other_core = {"gy_1": 1 - core}

    def block_of(slot, y):
        return 4 * (core + slot - 2 * core * slot) + lax.rem(y + 1, 4)


    def transposed(slot, y):
        at = 2 * y + slot
        first = pl.multiple_of(block_of(slot, y) * 256, 256)
        re_t = s[:DEPTH, pl.ds(first, 256)].T
        im_t = s[DEPTH:, pl.ds(first, 256)].T
        t[at, :, :DEPTH] = re_t
        t[at, :, DEPTH : 2 * DEPTH] = im_t
        t[at, :, 2 * DEPTH :] = -re_t

    def factor(slot, y, imag):
        return t[2 * y + slot, :, pl.ds(pl.multiple_of(imag * DEPTH, DEPTH), 2 * DEPTH)]

    def column(col):
        return s[:, pl.ds(pl.multiple_of(col * 256, 256), 256)]

    dot = functools.partial(jnp.dot, preferred_element_type=jnp.float32)

    def half_product(slot, dst, y, x, half):
        block, col = block_of(slot, y), 2 * x + half
        value = dot(factor(slot, y, (block - col + 7) // 8), column(col))
        for k in range(2):
            dst[y, x, 2 * half + k] = value[:, 128 * k : 128 * k + 128]

    def products(y, x):
        for half in range(2):
            col = 2 * x + half
            left = jnp.concatenate(
                [factor(slot, y, (block_of(slot, y) - col + 7) // 8) for slot in range(2)], axis=0
            )
            value = dot(left, column(col))
            for slot, dst in ((0, stage), (1, p)):
                for k in range(2):
                    dst[y, x, 2 * half + k] = value[
                        256 * slot : 256 * slot + 256, 128 * k : 128 * k + 128
                    ]

    def diagonal(slot, y):
        block = block_of(slot, y)
        imag = dot(factor(slot, y, 1), column(block))
        for k in range(2):
            lower[k] = imag[:, 128 * k : 128 * k + 128]

    def mend(y, x, slots=(0, 1)):
        row = lax.broadcasted_iota(jnp.int32, (256, 128), 0)
        lane = lax.broadcasted_iota(jnp.int32, (256, 128), 1)
        for slot in slots:
            dst = p if slot else stage
            block = block_of(slot, y)

            @pl.when(block // 2 == x)
            def _(dst=dst, block=block):
                for k in range(2):
                    z = 2 * lax.rem(block, 2) + k
                    dst[y, x, z] = jnp.where(lane + 128 * k >= row, dst[y, x, z], lower[k])

    def unit(y, x, beside=lambda: None):
        shift = block_of(0, y) // 2 - x

        @pl.when(lax.rem(shift + 4, 2) == 0)
        def _():
            products(y, x)
            diagonal(lax.rem(shift + 4, 4) // 2, y)
            beside()

        @pl.when(lax.rem(shift + 4, 2) != 0)
        def _():
            products(y, x)
            beside()

        mend(y, x)

    def unit_of(v):
        off_y, off_x = digit(UNITS_Y, v), digit(UNITS_X, v)
        return off_y, off_x, lax.rem(y0 + off_y, 4), lax.rem(x0 + off_x, 4)

    def core_copy(v, y, x):
        return remote(stage.at[y, x], cross.at[y, x], core_ss.at[0], core_rs.at[v], other_core)

    def core_half(y, x, half):
        return remote(
            stage.at[y, x, HALF[half]], cross.at[y, x, HALF[half]],
            core_ss.at[0], core_rs.at[16 * half], other_core,
        )

    def copy1(kind, o, src, key, index, step):
        line = index // 2 if o < 2 else index
        return remote(
            src,
            ph1.at[(kind,) + key + (ROWS[o],)],
            ss1.at[0],
            far1.at[BASE[o] + index] if kind == FAR else take_s.at[TAKE[o] + line],
            along[o](step),
        )

    def send1(kind, o, src, key, index, step):
        copy1(kind, o, src, key, index, step).start()

    def wait1(o, key, index):
        copy1(FAR, o, ph1.at[(FAR,) + key + (ROWS[o],)], key, index, 1).wait_recv()

    def add_cross(y, x):
        for z in range(4):
            p[y, x, z] += cross[y, x, z]

    def finish(v):
        off_y, off_x, y, x = unit_of(v)
        for o, off, line in ((0, off_x, y), (1, off_y, x)):
            @pl.when(off == 2)
            def _(o=o, line=line):
                for h, step in ((0, 1), (1, 3)):
                    send1(FAR, o, p.at[y, x, HALF[h], ROWS[o]], (line, HALF[h]), 2 * line + h, step)

            @pl.when(off == 1)
            def _(o=o, line=line):
                send1(PURE, o, p.at[y, x, HI, ROWS[o]], (line, HI), 2 * line + 1, 1)

            @pl.when(off == 3)
            def _(o=o, line=line):
                send1(PURE, o, p.at[y, x, LO, ROWS[o]], (line, LO), 2 * line, 3)

        up = lax.rem(v, 2)
        far, right, left = (lax.rem(z0 + k, 4) for k in (2, 1, 3))

        @pl.when(up == 0)
        def _():
            send1(FAR, 2, p.at[y, x, far, ROWS[2]], (y, x), 4 * y + x, 1)
            send1(PURE, 2, p.at[y, x, left, ROWS[2]], (y, x), 4 * y + x, 3)

        @pl.when(up == 1)
        def _():
            send1(FAR, 2, p.at[y, x, far, ROWS[2]], (y, x), 4 * y + x, 3)
            send1(PURE, 2, p.at[y, x, right, ROWS[2]], (y, x), 4 * y + x, 1)

    def forward_xy(v):
        off_y, off_x, y, x = unit_of(v)
        for o, off, line in ((0, off_x, y), (1, off_y, x)):
            for h, step in ((0, 1), (1, 3)):
                @pl.when(off == step)
                def _(o=o, line=line, h=h, step=step):
                    key, index = (line, HALF[h]), 2 * line + h
                    wait1(o, key, index)
                    p[y, x, HALF[h], ROWS[o]] += ph1[FAR, line, HALF[h], ROWS[o]]
                    send1(ACC, o, p.at[y, x, HALF[h], ROWS[o]], key, index, step)

    def forward_z(v):
        _, _, y, x = unit_of(v)
        wait1(2, (y, x), 4 * y + x)
        for h, step in ((0, 1), (1, 3)):
            @pl.when(lax.rem(v, 2) == h)
            def _(step=step):
                z = lax.rem(z0 + step, 4)
                p[y, x, z, ROWS[2]] += ph1[FAR, y, x, ROWS[2]]
                send1(ACC, 2, p.at[y, x, z, ROWS[2]], (y, x), 4 * y + x, step)

    def held(o, b, cs):
        if o == 0:
            return (b, x0, cs, ROWS[0])
        if o == 1:
            return (y0, cs, b, ROWS[1])
        return (cs, b, z0, ROWS[2])

    def landed(o, b, cs):
        return (b, cs, ROWS[0]) if o == 0 else (cs, b, ROWS[o])

    def at2(o, k):
        return lax.rem(origin2[o] + k, 4)

    def at3(o, k):
        return lax.rem(origin3[o] + k, 4)

    groups = ((((LO, 0, 0), (HI, 1, 1)),) + tuple(
        tuple((at3(o, k), n % 2, n) for n, k in enumerate((2, 3, 1, 0))) for o in (1, 2)
    ))

    def arrived(o, line):
        key = (line // 4, lax.rem(line, 4)) if o == 2 else (line, slice(None))
        ref = ph1.at[(slice(PURE, ACC + 1),) + key + (ROWS[o],)]
        remote(ref, ref, ss1.at[0], take_s.at[TAKE[o] + line], other_core).wait_recv()

    def add1(o, b, c):
        p[held(o, b, c)] += ph1[(PURE,) + landed(o, b, c)] + ph1[(ACC,) + landed(o, b, c)]

    def take0(b):
        arrived(0, b)
        for c in range(4):
            add1(0, b, c)

    def copy2(kind, o, src, group, step):
        cs, _, n = group
        return remote(
            src, ph2.at[kind, cs, ROWS[o]], ss2.at[0],
            far2.at[o, n] if kind == FAR else take2_s.at[o, n if o else 0], along2[o](step),
        )

    def wait2(o, group):
        copy2(FAR, o, ph2.at[FAR, group[0], ROWS[o]], group, 1).wait_recv()

    def send2(kind, o, group, step):
        b = at2(o, 2 if kind == FAR else step)
        copy2(kind, o, p.at[held(o, b, group[0])], group, step).start()

    UP = (1, 3)
    DOWN = (3, 1)

    def accumulate2(o, n):
        group = groups[o][n]
        cs, h, _ = group
        wait2(o, group)
        p[held(o, at2(o, UP[h]), cs)] += ph2[FAR, cs, ROWS[o]]
        send2(ACC, o, group, UP[h])

    def far0():
        take0(at2(0, 2))
        for group in groups[0]:
            send2(FAR, 0, group, UP[group[1]])

    def pure0(step):
        take0(at2(0, step))
        for group in groups[0]:
            if DOWN[group[1]] == step:
                send2(PURE, 0, group, step)

    def open2(o, n):
        group = groups[o][n]
        cs, h, _ = group

        def take(k):
            b = at2(o, k)
            if o == 2:
                arrived(2, 4 * cs + b)
            add1(o, b, cs)

        if o == 1:
            arrived(1, cs)
        take(2)
        send2(FAR, o, group, UP[h])
        take(DOWN[h])
        send2(PURE, o, group, DOWN[h])
        take(UP[h])

    def direct2(o, n):
        c = groups[o][n][0]
        if o == 1:
            arrived(1, c)
        for k in (2, 1, 3):
            b = at2(o, k)
            if o == 2:
                arrived(2, 4 * c + b)
            add1(o, b, c)
            remote(
                p.at[held(o, b, c)], ph2.at[k - 1, c, ROWS[o]],
                ss2.at[0], take2_s.at[o, n], along2[o](k),
            ).start()

    def own(o, c):
        return held(o, origin2[o], c)

    def send3(o, k):
        remote(
            p.at[own(o, at3(o, k))], ph3.at[k - 1, ROWS[o]], ss3.at[0], rs3.at[o], along3[o](k)
        ).start()

    def close2(o, n):
        c = groups[o][n][0]
        if o == 2:
            arrived(2, 4 * c + x0)
        add1(o, origin2[o], c)
        kinds = slice(PURE if n < 2 else FAR, ACC + 1)
        ref = ph2.at[kinds, c, ROWS[o]]
        remote(ref, ref, ss2.at[0], take2_s.at[o, n], other_core).wait_recv()
        total = ph2[PURE, c, ROWS[o]] + ph2[ACC, c, ROWS[o]]
        if n == 2:
            total = total + ph2[FAR, c, ROWS[o]]
        p[own(o, c)] += total
        send3(o, (2, 3, 1)[n])

    def close0():
        take0(y0)
        ref = ph2.at[PURE : ACC + 1, :, ROWS[0]]
        remote(ref, ref, ss2.at[0], take2_s.at[0, 0], other_core).wait_recv()
        for k in (2, 1, 3, 0):
            c = at3(0, k)
            p[own(0, c)] += ph2[PURE, c, ROWS[0]] + ph2[ACC, c, ROWS[0]]
            if k:
                send3(0, k)

    def share(pieces, first=False):
        runs = []
        for o, c in pieces:
            run = p[own(o, c)]
            row = ROWS[o].start + lax.broadcasted_iota(jnp.int32, run.shape, 0)
            lane = lax.broadcasted_iota(jnp.int32, run.shape, 1)
            runs.append((o, c, run, row, lane))
        moved = jnp.concatenate([run[2] for run in runs], axis=0)
        row = jnp.concatenate([run[3] for run in runs], axis=0)
        lane = jnp.concatenate([run[4] for run in runs], axis=0)
        for bit in range(7):
            hop = 1 << bit
            swapped = jnp.where(
                (lane & hop) != 0, pltpu.roll(moved, hop, 1), pltpu.roll(moved, 128 - hop, 1)
            )
            moved = jnp.where((row & hop) != 0, swapped, moved)
        high = moved.astype(jnp.bfloat16)
        rest = moved - high.astype(jnp.float32)
        middle = rest.astype(jnp.bfloat16)
        low = (rest - middle.astype(jnp.float32)).astype(jnp.bfloat16)
        read = dot(jnp.concatenate([high, middle, low], axis=1), pick[:, :TERMS])
        weight = jnp.concatenate([weights[c, ROWS[o], :TERMS] for o, c in pieces], axis=0)
        total = jnp.sum(weight * read, axis=0, keepdims=True)
        shares[:, :TERMS] = total if first else shares[:, :TERMS] + total

    def load(q):
        columns = pl.ds(pl.multiple_of(512 * q, 512), 512)
        return [
            pltpu.make_async_copy(
                amp.at[k, :, columns], s.at[pl.ds(DEPTH * k, DEPTH), columns], in_sem.at[2 * q + k]
            )
            for k in range(2)
        ]

    def start(q):
        for copy in load(q):
            copy.start()

    def loaded(q):
        for copy in load(q):
            copy.wait()

    first_y, first_x = lax.rem(y0 + 2, 4), lax.rem(x0 + 2, 4)
    chunk = block_of(0, first_y) // 2
    later = [lax.rem(chunk + k, 4) for k in (2, 1, 3)]
    start(chunk)
    pl.when(first_x != chunk)(lambda: start(first_x))
    for q in later:
        pl.when(first_x != q)(lambda q=q: start(q))
    terms = [
        pltpu.make_async_copy(src, dst, in_sem.at[8 + n])
        for n, (src, dst) in enumerate(((px_in, px), (pz_in, pz), (pph_in, pph)))
    ]
    for copy in terms:
        copy.start()
    barrier = pltpu.get_barrier_semaphore()
    partners = [other_core] + [f(k) for f in along for k in (1, 3)]
    for device in partners:
        pl.semaphore_signal(barrier, inc=1, device_id=device, device_id_type=pl.DeviceIdType.MESH)
    loaded(chunk)
    pl.when(first_x != chunk)(lambda: loaded(first_x))

    _, _, y, x = unit_of(0)
    transposed(0, y)
    half_product(0, stage, y, x, 0)
    half_product(0, stage, y, x, 1)
    pl.when(block_of(0, y) // 2 == x)(lambda: diagonal(0, y))
    mend(y, x, (0,))
    pl.semaphore_wait(barrier, len(partners))
    for half in range(2):
        core_half(y, x, half).start()
    for q in later:
        pl.when(first_x != q)(lambda q=q: loaded(q))
    for copy in terms:
        copy.wait()
    transposed(1, y)
    half_product(1, p, y, x, 0)
    half_product(1, p, y, x, 1)
    pl.when(block_of(1, y) // 2 == x)(lambda: diagonal(1, y))
    mend(y, x, (1,))
    _, _, next_y, next_x = unit_of(1)
    unit(next_y, next_x)
    core_copy(1, next_y, next_x).start()

    def settle(v):
        _, _, y, x = unit_of(v)
        core_copy(v, y, x).wait_recv()
        add_cross(y, x)
        finish(v)

    for half in range(2):
        core_half(y, x, half).wait_recv()
    for z in range(4):
        p[y, x, z] += cross[y, x, z]
    finish(0)
    _, _, y, x = unit_of(2)
    for slot in range(2):
        transposed(slot, y)
    unit(y, x)
    core_copy(2, y, x).start()

    def step(u, carry):
        off_y, off_x, y, x = unit_of(u)
        _, _, last_y, last_x = unit_of(u - 2)

        @pl.when(off_x == 2)
        def _():
            for slot in range(2):
                transposed(slot, y)
        core_copy(u - 2, last_y, last_x).wait_recv()
        unit(y, x, lambda: add_cross(last_y, last_x))
        core_copy(u, y, x).start()
        finish(u - 2)

        @pl.when(u >= 2 + LAG_Z)
        def _():
            forward_z(u - 2 - LAG_Z)

        @pl.when(u >= 2 + LAG_XY)
        def _():
            forward_xy(u - 2 - LAG_XY)

        @pl.when(u == 12)
        def _():
            open2(2, 0)

        @pl.when(u == 13)
        def _():
            far0()

        @pl.when(u == 15)
        def _():
            open2(1, 0)
            open2(2, 1)

        return carry

    lax.fori_loop(3, 16, step, 0)

    settle(14)
    forward_z(11)
    pure0(3)
    settle(15)
    forward_z(12)
    forward_xy(11)
    forward_z(13)
    forward_xy(13)
    accumulate2(2, 0)
    open2(1, 1)
    forward_z(14)
    forward_xy(14)
    forward_z(15)
    row_block = block_of(1, y0)
    col_block = 4 * x0 + z0
    xs, zs, phase = px[...], pz[...], pph[...]
    even = parity(xs & zs) == 0
    for n in range(3):
        rows = slice(128 * n, 128 * n + 128)
        pick[rows, :TERMS] = jnp.where(
            lax.broadcasted_iota(jnp.int32, (128, TERMS), 0) == (xs & 127), 1.0, 0.0
        ).astype(jnp.bfloat16)
    count = jnp.where(xs == 0, 1.0, 2.0) * (1.0 / COLS)
    row = lax.broadcasted_iota(jnp.int32, (256, TERMS), 0)
    for c in range(4):
        cols = jnp.where(row < 88, 4 * x0 + c, jnp.where(row < 176, 4 * c + z0, col_block))
        rows = 256 * jnp.where(row < 176, row_block, block_of(1, c)) + row
        sign = jnp.where(parity(rows & zs) == 0, count, -count)
        keep = ((rows ^ xs) >> 7) == cols
        weights[c, :, :TERMS] = jnp.where(
            keep & (((rows ^ xs) >= rows) == even), sign, 0.0
        )

    def phased(share):
        phase_re = jnp.where(phase == 0, 1.0, jnp.where(phase == 2, -1.0, 0.0))
        phase_im = jnp.where(phase == 1, 1.0, jnp.where(phase == 3, -1.0, 0.0))
        return share * jnp.concatenate(
            [jnp.where(even, phase_re, -phase_im), jnp.where(even, phase_im, phase_re)], axis=0
        )
    pure0(1)
    direct2(2, 2)
    direct2(1, 2)
    accumulate2(1, 0)
    accumulate2(2, 1)
    accumulate2(0, 1)
    accumulate2(0, 0)
    accumulate2(1, 1)
    close2(2, 0)
    direct2(2, 3)
    direct2(1, 3)
    close2(1, 0)
    close2(2, 1)
    close2(2, 2)
    close2(1, 1)
    close2(1, 2)
    share([(o, at3(o, k)) for o in (1, 2) for k in (2, 3, 1)], True)
    close0()
    for o in (1, 2):
        c = origin3[o]
        if o == 2:
            arrived(2, 4 * c + x0)
        add1(o, origin2[o], c)
        ref = ph2.at[:, c, ROWS[o]]
        remote(ref, ref, ss2.at[0], take2_s.at[o, 3], other_core).wait_recv()
        p[own(o, c)] += ph2[0, c, ROWS[o]] + ph2[1, c, ROWS[o]] + ph2[2, c, ROWS[o]]

    share([(0, c) for c in range(4)] + [(o, at3(o, 0)) for o in (1, 2)])
    here = shares[:, :TERMS]

    def give(here, parts, n, mine, count, where):
        parts[mine, :, :TERMS] = here
        for k in range(1, count):
            remote(
                parts.at[mine], parts.at[mine], ess.at[n], ers.at[n],
                where(lax.rem(mine + k, count)),
            ).start()

    def collect(parts, n, count):
        rest = parts.at[pl.ds(0, count - 1)]
        remote(rest, rest, ess.at[n], ers.at[n], other_core).wait_recv()
        total = parts[0, :, :TERMS]
        for k in range(1, count):
            total = total + parts[k, :, :TERMS]
        return total

    give(
        here, part0, 0, 4 * x0 + z0, 16,
        lambda k: {"gx": k // 4, "gy_0": lax.rem(k // 2, 2), "gz_1": lax.rem(k, 2)},
    )

    for o in range(3):
        ref = ph3.at[:, ROWS[o]]
        remote(ref, ref, ss3.at[0], rs3.at[o], other_core).wait_recv()
    block = p[y0, x0, z0] + ph3[0] + ph3[1] + ph3[2]
    p[y0, x0, z0] = block

    flipped[...] = block.T

    def device(e):
        return {
            "gx": e // 32,
            "gy_0": lax.rem(e // 16, 2),
            "gy_1": lax.rem(e // 8, 2),
            "gz_0": lax.rem(e // 2, 4),
            "gz_1": lax.rem(e, 2),
        }

    def direct_copy(k):
        e = 16 * row_block + k
        return e, remote(
            p.at[y0, x0, z0, pl.ds(16 * k, 16)], direct.at[col_block],
            dss.at[0], drs.at[0], device(e),
        )

    def mirror_copy(k):
        e = 8 * col_block + k
        return e, remote(
            flipped.at[pl.ds(16 * k, 16)], mirror.at[row_block],
            mss.at[0], mrs.at[0], device(e),
        )

    @pl.when(me // 16 != row_block)
    def _():
        for k in range(16):
            direct_copy(k)[1].start()

    @pl.when(me // 16 == row_block)
    def _():
        for k in range(16):
            e, copy = direct_copy(k)
            pl.when(e != me)(copy.start)

            @pl.when(e == me)
            def _(k=k):
                direct[col_block] = p[y0, x0, z0, pl.ds(16 * k, 16)]

    @pl.when(me // 8 != col_block)
    def _():
        for k in range(8):
            mirror_copy(k)[1].start()

    @pl.when(me // 8 == col_block)
    def _():
        for k in range(8):
            e, copy = mirror_copy(k)
            pl.when(e != me)(copy.start)

            @pl.when(e == me)
            def _(k=k):
                mirror[row_block] = flipped[pl.ds(16 * k, 16)]

    give(
        collect(part0, 0, 16), part1, 1, 2 * y0 + core, 8,
        lambda k: {"gz_0": k // 2, "gy_1": lax.rem(k, 2)},
    )
    out_ex[...] = phased(collect(part1, 1, 8))

    def landed_and_left(ref, ss, rs):
        copy = remote(ref, ref, ss, rs, other_core)
        copy.wait_recv()
        copy.wait_send()

    @pl.when(me // 16 == row_block)
    def _():
        landed_and_left(direct.at[pl.ds(0, 15)], dss.at[0], drs.at[0])

    @pl.when(me // 16 != row_block)
    def _():
        landed_and_left(direct, dss.at[0], drs.at[0])

    @pl.when(me // 8 == col_block)
    def _():
        landed_and_left(mirror.at[pl.ds(0, 7)], mss.at[0], mrs.at[0])

    @pl.when(me // 8 != col_block)
    def _():
        landed_and_left(mirror, mss.at[0], mrs.at[0])

    row = 16 * me + lax.broadcasted_iota(jnp.int32, (16, 128), 0)
    lane = lax.broadcasted_iota(jnp.int32, (16, 128), 1)
    for k in range(16):
        given = direct[k] * (1.0 / COLS)
        turned = mirror[k // 2, :, 128 * (k % 2) : 128 * (k % 2) + 128] * (1.0 / COLS)
        col = 128 * k + lane
        out_re[:, 128 * k : 128 * k + 128] = jnp.where(col >= row, given, turned)
        out_im[:, 128 * k : 128 * k + 128] = jnp.where(
            col < row, given, jnp.where(col == row, 0.0, -turned)
        )

    def left(ref, sem):
        remote(ref, ref, sem, core_rs.at[0], other_core).wait_send()

    left(stage, core_ss.at[0])
    left(ph1, ss1.at[0])
    left(ph2, ss2.at[0])
    left(ph3, ss3.at[0])
    left(part0.at[pl.ds(0, 15)], ess.at[0])
    left(part1.at[pl.ds(0, 7)], ess.at[1])


def put_out(re, im, ex, out_re, out_im, out_ex):
    out_re[...] = re[...]
    out_im[...] = im[...]
    out_ex[...] = ex[...]


def on_device(amplitudes, pauli_x, pauli_z, pauli_phase):
    vmem = pl.BlockSpec(memory_space=pltpu.VMEM)
    f32 = jnp.float32
    dma = pltpu.SemaphoreType.DMA
    results = pl.pallas_call(
        kernel,
        out_shape=(
            jax.ShapeDtypeStruct((16, ORDER), f32),
            jax.ShapeDtypeStruct((16, ORDER), f32),
            jax.ShapeDtypeStruct((2, TERMS), f32),
        ),
        in_specs=[pl.BlockSpec(memory_space=pltpu.HBM)] * 4,
        out_specs=(vmem, vmem, vmem),
        scratch_shapes=[
            pltpu.VMEM((2 * DEPTH, ORDER), jnp.bfloat16),
            pltpu.VMEM((8, 256, 3 * DEPTH), jnp.bfloat16),
            pltpu.VMEM((2, 256, 128), f32),
            pltpu.VMEM((4, 4, 4, 256, 128), f32),
            pltpu.VMEM((4, 4, 4, 256, 128), f32),
            pltpu.VMEM((4, 4, 4, 256, 128), f32),
            pltpu.VMEM((3, 4, 4, 256, 128), f32),
            pltpu.VMEM((3, 4, 256, 128), f32),
            pltpu.VMEM((3, 256, 128), f32),
            pltpu.VMEM((128, 256), f32),
            pltpu.VMEM((16, 16, 128), f32),
            pltpu.VMEM((8, 16, 256), f32),
            pltpu.VMEM((4, 256, TERMS_PAD), f32),
            pltpu.VMEM((384, TERMS_PAD), jnp.bfloat16),
            pltpu.VMEM((1, TERMS_PAD), f32),
            pltpu.VMEM((16, 1, TERMS_PAD), f32),
            pltpu.VMEM((8, 1, TERMS_PAD), f32),
            pltpu.VMEM((1, TERMS), jnp.int32),
            pltpu.VMEM((1, TERMS), jnp.int32),
            pltpu.VMEM((1, TERMS), jnp.int32),
            dma((11,)),
            dma((1,)),
            dma((17,)),
            dma((1,)),
            dma((32,)),
            dma((24,)),
            dma((1,)),
            dma((3, 4)),
            dma((3, 4)),
            dma((1,)),
            dma((3,)),
            dma((1,)),
            dma((1,)),
            dma((1,)),
            dma((1,)),
            dma((2,)),
            dma((2,)),
        ],
        compiler_params=pltpu.CompilerParams(
            collective_id=0, has_side_effects=True, vmem_limit_bytes=50 * 1024 * 1024
        ),
    )(*(pltpu.with_memory_space_constraint(v, pltpu.HBM) for v in (amplitudes, pauli_x.reshape(1, TERMS), pauli_z.reshape(1, TERMS), pauli_phase.reshape(1, TERMS))))
    return pl.pallas_call(
        put_out,
        out_shape=tuple(jax.ShapeDtypeStruct(r.shape, f32) for r in results),
        in_specs=[vmem] * 3,
        out_specs=(vmem,) * 3,
        compiler_params=pltpu.CompilerParams(vmem_limit_bytes=4 * 1024 * 1024),
    )(*results)


def solution(mesh):
    finer = Mesh(mesh.devices.reshape(mesh.shape["gx"], 2, 2, 4, 2), AXES)
    return jax.shard_map(
        on_device,
        mesh=finer,
        in_specs=(P(None, AXES, None), P(), P(), P()),
        out_specs=(P(AXES, None), P(AXES, None), P()),
        check_vma=False,
    )
```

```python
import functools

import jax
import jax.numpy as jnp
from jax import lax
from jax.experimental import pallas as pl
from jax.experimental.pallas import tpu as pltpu
from jax.sharding import Mesh
from jax.sharding import PartitionSpec as P

ORDER = 2048
COLS = 65536
DEPTH = 512
TERMS = 200
TERMS_PAD = 256
AXES = ("gx", "gy_0", "gy_1", "gz_0", "gz_1")
ROWS = (slice(0, 88), slice(88, 176), slice(176, 256))
FAR, PURE, ACC = 0, 1, 2
LAG_Z, LAG_XY = 4, 4
BASE = (0, 8, 16)
TAKE = (0, 4, 8)
UNITS = (
    (2, 2), (2, 3), (3, 2), (2, 1), (1, 2), (3, 3), (3, 1), (1, 3),
    (1, 1), (2, 0), (3, 0), (1, 0), (0, 2), (0, 3), (0, 1), (0, 0),
)
LO, HI = slice(0, 2), slice(2, 4)
HALF = (LO, HI)


def remote(src, dst, send, recv, device):
    return pltpu.make_async_remote_copy(
        src_ref=src,
        dst_ref=dst,
        send_sem=send,
        recv_sem=recv,
        device_id=device,
        device_id_type=pl.DeviceIdType.MESH,
    )


def parity(values):
    values = values ^ (values >> 8)
    values = values ^ (values >> 4)
    values = values ^ (values >> 2)
    values = values ^ (values >> 1)
    return values & 1


def kernel(
    amp, px_in, pz_in, pph_in,
    out_re, out_im, out_ex,
    s, t0, t1, t2, t3, lower, p, stage, cross, ph1, ph2, ph3, flipped, direct, mirror, weights, pick, shares, part0, part1,
    px, pz, pph, in_sem, core_ss, core_rs, ss1, far1, take_s, ss2, far2, take2_s, ss3, rs3,
    dss, drs, mss, mrs, ess, ers,
):
    x0 = lax.axis_index("gx")
    zh = lax.axis_index("gy_0")
    core = lax.axis_index("gy_1")
    y0 = lax.axis_index("gz_0")
    zl = lax.axis_index("gz_1")
    z0 = 2 * zh + zl
    me = x0 * 32 + zh * 16 + core * 8 + y0 * 2 + zl

    def at_x(step):
        return {"gx": lax.rem(x0 + step, 4)}

    def at_y(step):
        return {"gz_0": lax.rem(y0 + step, 4)}

    def at_z(step):
        z = lax.rem(z0 + step, 4)
        return {"gy_0": z // 2, "gz_1": lax.rem(z, 2)}

    along = (at_x, at_y, at_z)
    along2 = (at_y, at_z, at_x)
    along3 = (at_z, at_x, at_y)
    origin2 = (y0, z0, x0)
    origin3 = (z0, x0, y0)
    other_core = {"gy_1": 1 - core}

    def block_of(slot, y):
        return 4 * (core + slot - 2 * core * slot) + lax.rem(y + 1, 4)


    flips = (t0, t1, t2, t3)

    def at_offset(off_y):
        return lax.rem(y0 + off_y, 4)

    def transposed(slot, off_y):
        t = flips[off_y]
        first = pl.multiple_of(block_of(slot, at_offset(off_y)) * 256, 256)
        re_t = s[:DEPTH, pl.ds(first, 256)].T
        im_t = s[DEPTH:, pl.ds(first, 256)].T
        t[slot, :, :DEPTH] = re_t
        t[slot, :, DEPTH : 2 * DEPTH] = im_t
        t[slot, :, 2 * DEPTH :] = -re_t

    def factor(slot, off_y, imag):
        return flips[off_y][slot, :, pl.ds(pl.multiple_of(imag * DEPTH, DEPTH), 2 * DEPTH)]

    def column(col):
        return s[:, pl.ds(pl.multiple_of(col * 256, 256), 256)]

    dot = functools.partial(jnp.dot, preferred_element_type=jnp.float32)

    def half_product(slot, dst, off_y, x, half):
        y = at_offset(off_y)
        block, col = block_of(slot, y), 2 * x + half
        value = dot(factor(slot, off_y, (block - col + 7) // 8), column(col))
        for k in range(2):
            dst[y, x, 2 * half + k] = value[:, 128 * k : 128 * k + 128]

    def products(off_y, x):
        y = at_offset(off_y)
        for half in range(2):
            col = 2 * x + half
            left = jnp.concatenate(
                [
                    factor(slot, off_y, (block_of(slot, y) - col + 7) // 8)
                    for slot in range(2)
                ],
                axis=0,
            )
            value = dot(left, column(col))
            for slot, dst in ((0, stage), (1, p)):
                for k in range(2):
                    dst[y, x, 2 * half + k] = value[
                        256 * slot : 256 * slot + 256, 128 * k : 128 * k + 128
                    ]

    def diagonal(slot, off_y):
        imag = dot(factor(slot, off_y, 1), column(block_of(slot, at_offset(off_y))))
        for k in range(2):
            lower[k] = imag[:, 128 * k : 128 * k + 128]

    def mend(y, x, slots=(0, 1)):
        row = lax.broadcasted_iota(jnp.int32, (256, 128), 0)
        lane = lax.broadcasted_iota(jnp.int32, (256, 128), 1)
        for slot in slots:
            dst = p if slot else stage
            block = block_of(slot, y)

            @pl.when(block // 2 == x)
            def _(dst=dst, block=block):
                for k in range(2):
                    z = 2 * lax.rem(block, 2) + k
                    dst[y, x, z] = jnp.where(lane + 128 * k >= row, dst[y, x, z], lower[k])

    def unit(v, beside=lambda: None):
        off_y, _, y, x = unit_of(v)
        shift = block_of(0, y) // 2 - x

        @pl.when(lax.rem(shift + 4, 2) == 0)
        def _():
            products(off_y, x)
            diagonal(lax.rem(shift + 4, 4) // 2, off_y)
            beside()

        @pl.when(lax.rem(shift + 4, 2) != 0)
        def _():
            products(off_y, x)
            beside()

        mend(y, x)
        if v:
            core_copy(v, y, x).start()

    def unit_of(v):
        off_y, off_x = UNITS[v]
        return off_y, off_x, lax.rem(y0 + off_y, 4), lax.rem(x0 + off_x, 4)

    def core_copy(v, y, x):
        return remote(stage.at[y, x], cross.at[y, x], core_ss.at[0], core_rs.at[v], other_core)

    def core_half(y, x, half):
        return remote(
            stage.at[y, x, HALF[half]], cross.at[y, x, HALF[half]],
            core_ss.at[0], core_rs.at[16 * half], other_core,
        )

    def copy1(kind, o, src, key, index, step):
        line = index // 2 if o < 2 else index
        return remote(
            src,
            ph1.at[(kind,) + key + (ROWS[o],)],
            ss1.at[0],
            far1.at[BASE[o] + index] if kind == FAR else take_s.at[TAKE[o] + line],
            along[o](step),
        )

    def send1(kind, o, src, key, index, step):
        copy1(kind, o, src, key, index, step).start()

    def wait1(o, key, index):
        copy1(FAR, o, ph1.at[(FAR,) + key + (ROWS[o],)], key, index, 1).wait_recv()

    def add_cross(y, x):
        for z in range(4):
            p[y, x, z] += cross[y, x, z]

    def finish(v):
        off_y, off_x, y, x = unit_of(v)
        for o, off, line in ((0, off_x, y), (1, off_y, x)):
            @pl.when(off == 2)
            def _(o=o, line=line):
                for h, step in ((0, 1), (1, 3)):
                    send1(FAR, o, p.at[y, x, HALF[h], ROWS[o]], (line, HALF[h]), 2 * line + h, step)

            @pl.when(off == 1)
            def _(o=o, line=line):
                send1(PURE, o, p.at[y, x, HI, ROWS[o]], (line, HI), 2 * line + 1, 1)

            @pl.when(off == 3)
            def _(o=o, line=line):
                send1(PURE, o, p.at[y, x, LO, ROWS[o]], (line, LO), 2 * line, 3)

        up = v % 2
        far, right, left = (lax.rem(z0 + k, 4) for k in (2, 1, 3))

        @pl.when(up == 0)
        def _():
            send1(FAR, 2, p.at[y, x, far, ROWS[2]], (y, x), 4 * y + x, 1)
            send1(PURE, 2, p.at[y, x, left, ROWS[2]], (y, x), 4 * y + x, 3)

        @pl.when(up == 1)
        def _():
            send1(FAR, 2, p.at[y, x, far, ROWS[2]], (y, x), 4 * y + x, 3)
            send1(PURE, 2, p.at[y, x, right, ROWS[2]], (y, x), 4 * y + x, 1)

    def forward_xy(v):
        off_y, off_x, y, x = unit_of(v)
        for o, off, line in ((0, off_x, y), (1, off_y, x)):
            for h, step in ((0, 1), (1, 3)):
                @pl.when(off == step)
                def _(o=o, line=line, h=h, step=step):
                    key, index = (line, HALF[h]), 2 * line + h
                    wait1(o, key, index)
                    p[y, x, HALF[h], ROWS[o]] += ph1[FAR, line, HALF[h], ROWS[o]]
                    send1(ACC, o, p.at[y, x, HALF[h], ROWS[o]], key, index, step)

    def forward_z(v):
        _, _, y, x = unit_of(v)
        wait1(2, (y, x), 4 * y + x)
        for h, step in ((0, 1), (1, 3)):
            @pl.when(v % 2 == h)
            def _(step=step):
                z = lax.rem(z0 + step, 4)
                p[y, x, z, ROWS[2]] += ph1[FAR, y, x, ROWS[2]]
                send1(ACC, 2, p.at[y, x, z, ROWS[2]], (y, x), 4 * y + x, step)

    def held(o, b, cs):
        if o == 0:
            return (b, x0, cs, ROWS[0])
        if o == 1:
            return (y0, cs, b, ROWS[1])
        return (cs, b, z0, ROWS[2])

    def landed(o, b, cs):
        return (b, cs, ROWS[0]) if o == 0 else (cs, b, ROWS[o])

    def at2(o, k):
        return lax.rem(origin2[o] + k, 4)

    def at3(o, k):
        return lax.rem(origin3[o] + k, 4)

    groups = ((((LO, 0, 0), (HI, 1, 1)),) + tuple(
        tuple((at3(o, k), n % 2, n) for n, k in enumerate((2, 3, 1, 0))) for o in (1, 2)
    ))

    def arrived(o, line):
        key = (line // 4, lax.rem(line, 4)) if o == 2 else (line, slice(None))
        ref = ph1.at[(slice(PURE, ACC + 1),) + key + (ROWS[o],)]
        remote(ref, ref, ss1.at[0], take_s.at[TAKE[o] + line], other_core).wait_recv()

    def add1(o, b, c):
        p[held(o, b, c)] += ph1[(PURE,) + landed(o, b, c)] + ph1[(ACC,) + landed(o, b, c)]

    def take0(b):
        arrived(0, b)
        for c in range(4):
            add1(0, b, c)

    def copy2(kind, o, src, group, step):
        cs, _, n = group
        return remote(
            src, ph2.at[kind, cs, ROWS[o]], ss2.at[0],
            far2.at[o, n] if kind == FAR else take2_s.at[o, n if o else 0], along2[o](step),
        )

    def wait2(o, group):
        copy2(FAR, o, ph2.at[FAR, group[0], ROWS[o]], group, 1).wait_recv()

    def send2(kind, o, group, step):
        b = at2(o, 2 if kind == FAR else step)
        copy2(kind, o, p.at[held(o, b, group[0])], group, step).start()

    UP = (1, 3)
    DOWN = (3, 1)

    def accumulate2(o, n):
        group = groups[o][n]
        cs, h, _ = group
        wait2(o, group)
        p[held(o, at2(o, UP[h]), cs)] += ph2[FAR, cs, ROWS[o]]
        send2(ACC, o, group, UP[h])

    def far0():
        take0(at2(0, 2))
        for group in groups[0]:
            send2(FAR, 0, group, UP[group[1]])

    def pure0(step):
        take0(at2(0, step))
        for group in groups[0]:
            if DOWN[group[1]] == step:
                send2(PURE, 0, group, step)

    def open2(o, n):
        group = groups[o][n]
        cs, h, _ = group

        def take(k):
            b = at2(o, k)
            if o == 2:
                arrived(2, 4 * cs + b)
            add1(o, b, cs)

        if o == 1:
            arrived(1, cs)
        take(2)
        send2(FAR, o, group, UP[h])
        take(DOWN[h])
        send2(PURE, o, group, DOWN[h])
        take(UP[h])

    def direct2(o, n):
        c = groups[o][n][0]
        if o == 1:
            arrived(1, c)
        for k in (2, 1, 3):
            b = at2(o, k)
            if o == 2:
                arrived(2, 4 * c + b)
            add1(o, b, c)
            remote(
                p.at[held(o, b, c)], ph2.at[k - 1, c, ROWS[o]],
                ss2.at[0], take2_s.at[o, n], along2[o](k),
            ).start()

    def own(o, c):
        return held(o, origin2[o], c)

    def send3(o, k):
        remote(
            p.at[own(o, at3(o, k))], ph3.at[k - 1, ROWS[o]], ss3.at[0], rs3.at[o], along3[o](k)
        ).start()

    def close2(o, n):
        c = groups[o][n][0]
        if o == 2:
            arrived(2, 4 * c + x0)
        add1(o, origin2[o], c)
        kinds = slice(PURE if n < 2 else FAR, ACC + 1)
        ref = ph2.at[kinds, c, ROWS[o]]
        remote(ref, ref, ss2.at[0], take2_s.at[o, n], other_core).wait_recv()
        total = ph2[PURE, c, ROWS[o]] + ph2[ACC, c, ROWS[o]]
        if n == 2:
            total = total + ph2[FAR, c, ROWS[o]]
        p[own(o, c)] += total
        send3(o, (2, 3, 1)[n])

    def close0():
        take0(y0)
        ref = ph2.at[PURE : ACC + 1, :, ROWS[0]]
        remote(ref, ref, ss2.at[0], take2_s.at[0, 0], other_core).wait_recv()
        for k in (2, 1, 3, 0):
            c = at3(0, k)
            p[own(0, c)] += ph2[PURE, c, ROWS[0]] + ph2[ACC, c, ROWS[0]]
            if k:
                send3(0, k)

    def share(pieces, first=False):
        runs = []
        for o, c in pieces:
            run = p[own(o, c)]
            row = ROWS[o].start + lax.broadcasted_iota(jnp.int32, run.shape, 0)
            lane = lax.broadcasted_iota(jnp.int32, run.shape, 1)
            runs.append((o, c, run, row, lane))
        moved = jnp.concatenate([run[2] for run in runs], axis=0)
        row = jnp.concatenate([run[3] for run in runs], axis=0)
        lane = jnp.concatenate([run[4] for run in runs], axis=0)
        for bit in range(7):
            hop = 1 << bit
            swapped = jnp.where(
                (lane & hop) != 0, pltpu.roll(moved, hop, 1), pltpu.roll(moved, 128 - hop, 1)
            )
            moved = jnp.where((row & hop) != 0, swapped, moved)
        high = moved.astype(jnp.bfloat16)
        rest = moved - high.astype(jnp.float32)
        middle = rest.astype(jnp.bfloat16)
        low = (rest - middle.astype(jnp.float32)).astype(jnp.bfloat16)
        read = dot(jnp.concatenate([high, middle, low], axis=1), pick[:, :TERMS])
        weight = jnp.concatenate([weights[c, ROWS[o], :TERMS] for o, c in pieces], axis=0)
        total = jnp.sum(weight * read, axis=0, keepdims=True)
        shares[:, :TERMS] = total if first else shares[:, :TERMS] + total

    def load(q):
        columns = pl.ds(pl.multiple_of(512 * q, 512), 512)
        return [
            pltpu.make_async_copy(
                amp.at[k, :, columns], s.at[pl.ds(DEPTH * k, DEPTH), columns], in_sem.at[2 * q + k]
            )
            for k in range(2)
        ]

    def start(q):
        for copy in load(q):
            copy.start()

    def loaded(q):
        for copy in load(q):
            copy.wait()

    first_y, first_x = lax.rem(y0 + 2, 4), lax.rem(x0 + 2, 4)
    chunk = block_of(0, first_y) // 2
    later = [lax.rem(chunk + k, 4) for k in (2, 1, 3)]
    start(chunk)
    pl.when(first_x != chunk)(lambda: start(first_x))
    for q in later:
        pl.when(first_x != q)(lambda q=q: start(q))
    terms = [
        pltpu.make_async_copy(src, dst, in_sem.at[8 + n])
        for n, (src, dst) in enumerate(((px_in, px), (pz_in, pz), (pph_in, pph)))
    ]
    for copy in terms:
        copy.start()
    barrier = pltpu.get_barrier_semaphore()
    partners = [other_core] + [f(k) for f in along for k in (1, 3)]
    for device in partners:
        pl.semaphore_signal(barrier, inc=1, device_id=device, device_id_type=pl.DeviceIdType.MESH)
    loaded(chunk)
    pl.when(first_x != chunk)(lambda: loaded(first_x))

    _, _, y, x = unit_of(0)
    transposed(0, 2)
    half_product(0, stage, 2, x, 0)
    half_product(0, stage, 2, x, 1)
    pl.when(block_of(0, y) // 2 == x)(lambda: diagonal(0, 2))
    mend(y, x, (0,))
    pl.semaphore_wait(barrier, len(partners))
    for half in range(2):
        core_half(y, x, half).start()
    for q in later:
        pl.when(first_x != q)(lambda q=q: loaded(q))
    for copy in terms:
        copy.wait()
    transposed(1, 2)
    half_product(1, p, 2, x, 0)
    half_product(1, p, 2, x, 1)
    pl.when(block_of(1, y) // 2 == x)(lambda: diagonal(1, 2))
    mend(y, x, (1,))

    def turned(off_y):
        for slot in range(2):
            transposed(slot, off_y)

    unit(1, lambda: turned(3))

    def settle(v):
        _, _, y, x = unit_of(v)
        core_copy(v, y, x).wait_recv()
        add_cross(y, x)
        finish(v)

    for half in range(2):
        core_half(y, x, half).wait_recv()
    add_cross(y, x)
    finish(0)
    unit(2)

    for u in range(3, 16):
        _, _, last_y, last_x = unit_of(u - 2)
        core_copy(u - 2, last_y, last_x).wait_recv()

        def beside(u=u, last_y=last_y, last_x=last_x):
            add_cross(last_y, last_x)
            if u in (3, 7):
                turned(1 if u == 3 else 0)

        unit(u, beside)
        finish(u - 2)
        if u >= 2 + LAG_Z:
            forward_z(u - 2 - LAG_Z)
        if u >= 2 + LAG_XY:
            forward_xy(u - 2 - LAG_XY)
        if u == 13:
            open2(2, 0)
        if u == 14:
            far0()

    settle(14)
    forward_z(10)
    forward_xy(10)
    settle(15)
    forward_z(11)
    forward_xy(11)
    forward_z(12)
    pure0(3)
    open2(1, 0)
    forward_z(13)
    forward_xy(13)
    accumulate2(2, 0)
    open2(2, 1)
    open2(1, 1)
    forward_z(14)
    forward_xy(14)
    forward_z(15)
    row_block = block_of(1, y0)
    col_block = 4 * x0 + z0
    xs, zs, phase = px[...], pz[...], pph[...]
    even = parity(xs & zs) == 0
    for n in range(3):
        rows = slice(128 * n, 128 * n + 128)
        pick[rows, :TERMS] = jnp.where(
            lax.broadcasted_iota(jnp.int32, (128, TERMS), 0) == (xs & 127), 1.0, 0.0
        ).astype(jnp.bfloat16)
    count = jnp.where(xs == 0, 1.0, 2.0) * (1.0 / COLS)
    row = lax.broadcasted_iota(jnp.int32, (256, TERMS), 0)
    for c in range(4):
        cols = jnp.where(row < 88, 4 * x0 + c, jnp.where(row < 176, 4 * c + z0, col_block))
        rows = 256 * jnp.where(row < 176, row_block, block_of(1, c)) + row
        sign = jnp.where(parity(rows & zs) == 0, count, -count)
        keep = ((rows ^ xs) >> 7) == cols
        weights[c, :, :TERMS] = jnp.where(
            keep & (((rows ^ xs) >= rows) == even), sign, 0.0
        )

    def phased(share):
        phase_re = jnp.where(phase == 0, 1.0, jnp.where(phase == 2, -1.0, 0.0))
        phase_im = jnp.where(phase == 1, 1.0, jnp.where(phase == 3, -1.0, 0.0))
        return share * jnp.concatenate(
            [jnp.where(even, phase_re, -phase_im), jnp.where(even, phase_im, phase_re)], axis=0
        )
    pure0(1)
    direct2(2, 2)
    direct2(1, 2)
    accumulate2(1, 0)
    accumulate2(2, 1)
    accumulate2(0, 1)
    accumulate2(0, 0)
    accumulate2(1, 1)
    close2(2, 0)
    direct2(2, 3)
    direct2(1, 3)
    close2(2, 1)
    close2(1, 0)
    close2(2, 2)
    close2(1, 1)
    close2(1, 2)
    share([(o, at3(o, k)) for o in (1, 2) for k in (2, 3, 1)], True)
    close0()
    for o in (1, 2):
        c = origin3[o]
        if o == 2:
            arrived(2, 4 * c + x0)
        add1(o, origin2[o], c)
        ref = ph2.at[:, c, ROWS[o]]
        remote(ref, ref, ss2.at[0], take2_s.at[o, 3], other_core).wait_recv()
        p[own(o, c)] += ph2[0, c, ROWS[o]] + ph2[1, c, ROWS[o]] + ph2[2, c, ROWS[o]]

    share([(0, c) for c in range(4)] + [(o, at3(o, 0)) for o in (1, 2)])
    here = shares[:, :TERMS]

    def give(here, parts, n, mine, count, where):
        parts[mine, :, :TERMS] = here
        for k in range(1, count):
            remote(
                parts.at[mine], parts.at[mine], ess.at[n], ers.at[n],
                where(lax.rem(mine + k, count)),
            ).start()

    def collect(parts, n, count):
        rest = parts.at[pl.ds(0, count - 1)]
        remote(rest, rest, ess.at[n], ers.at[n], other_core).wait_recv()
        total = parts[0, :, :TERMS]
        for k in range(1, count):
            total = total + parts[k, :, :TERMS]
        return total

    give(
        here, part0, 0, 4 * x0 + z0, 16,
        lambda k: {"gx": k // 4, "gy_0": lax.rem(k // 2, 2), "gz_1": lax.rem(k, 2)},
    )

    for o in range(3):
        ref = ph3.at[:, ROWS[o]]
        remote(ref, ref, ss3.at[0], rs3.at[o], other_core).wait_recv()
    block = p[y0, x0, z0] + ph3[0] + ph3[1] + ph3[2]
    p[y0, x0, z0] = block

    flipped[...] = block.T

    def device(e):
        return {
            "gx": e // 32,
            "gy_0": lax.rem(e // 16, 2),
            "gy_1": lax.rem(e // 8, 2),
            "gz_0": lax.rem(e // 2, 4),
            "gz_1": lax.rem(e, 2),
        }

    def direct_copy(k):
        e = 16 * row_block + k
        return e, remote(
            p.at[y0, x0, z0, pl.ds(16 * k, 16)], direct.at[col_block],
            dss.at[0], drs.at[0], device(e),
        )

    def mirror_copy(k):
        e = 8 * col_block + k
        return e, remote(
            flipped.at[pl.ds(16 * k, 16)], mirror.at[row_block],
            mss.at[0], mrs.at[0], device(e),
        )

    far_first = [
        8 * half + 2 * lax.rem(y0 + k, 4) + low
        for half in range(2) for k in (2, 3, 1, 0) for low in range(2)
    ]
    @pl.when(me // 16 != row_block)
    def _():
        for k in far_first:
            direct_copy(k)[1].start()

    @pl.when(me // 16 == row_block)
    def _():
        for k in range(16):
            e, copy = direct_copy(k)
            pl.when(e != me)(copy.start)

            @pl.when(e == me)
            def _(k=k):
                direct[col_block] = p[y0, x0, z0, pl.ds(16 * k, 16)]

    @pl.when(me // 8 != col_block)
    def _():
        for k in far_first[:8]:
            mirror_copy(k)[1].start()

    @pl.when(me // 8 == col_block)
    def _():
        for k in range(8):
            e, copy = mirror_copy(k)
            pl.when(e != me)(copy.start)

            @pl.when(e == me)
            def _(k=k):
                mirror[row_block] = flipped[pl.ds(16 * k, 16)]

    give(
        collect(part0, 0, 16), part1, 1, 2 * y0 + core, 8,
        lambda k: {"gz_0": k // 2, "gy_1": lax.rem(k, 2)},
    )
    out_ex[...] = phased(collect(part1, 1, 8))

    def landed_and_left(ref, ss, rs):
        copy = remote(ref, ref, ss, rs, other_core)
        copy.wait_recv()
        copy.wait_send()

    @pl.when(me // 16 == row_block)
    def _():
        landed_and_left(direct.at[pl.ds(0, 15)], dss.at[0], drs.at[0])

    @pl.when(me // 16 != row_block)
    def _():
        landed_and_left(direct, dss.at[0], drs.at[0])

    @pl.when(me // 8 == col_block)
    def _():
        landed_and_left(mirror.at[pl.ds(0, 7)], mss.at[0], mrs.at[0])

    @pl.when(me // 8 != col_block)
    def _():
        landed_and_left(mirror, mss.at[0], mrs.at[0])

    row = 16 * me + lax.broadcasted_iota(jnp.int32, (16, 128), 0)
    lane = lax.broadcasted_iota(jnp.int32, (16, 128), 1)
    for k in range(16):
        given = direct[k] * (1.0 / COLS)
        turned = mirror[k // 2, :, 128 * (k % 2) : 128 * (k % 2) + 128] * (1.0 / COLS)
        col = 128 * k + lane
        out_re[:, 128 * k : 128 * k + 128] = jnp.where(col >= row, given, turned)
        out_im[:, 128 * k : 128 * k + 128] = jnp.where(
            col < row, given, jnp.where(col == row, 0.0, -turned)
        )

    def left(ref, sem):
        remote(ref, ref, sem, core_rs.at[0], other_core).wait_send()

    left(stage, core_ss.at[0])
    left(ph1, ss1.at[0])
    left(ph2, ss2.at[0])
    left(ph3, ss3.at[0])
    left(part0.at[pl.ds(0, 15)], ess.at[0])
    left(part1.at[pl.ds(0, 7)], ess.at[1])


def put_out(re, im, ex, out_re, out_im, out_ex):
    out_re[...] = re[...]
    out_im[...] = im[...]
    out_ex[...] = ex[...]


def on_device(amplitudes, pauli_x, pauli_z, pauli_phase):
    vmem = pl.BlockSpec(memory_space=pltpu.VMEM)
    f32 = jnp.float32
    dma = pltpu.SemaphoreType.DMA
    results = pl.pallas_call(
        kernel,
        out_shape=(
            jax.ShapeDtypeStruct((16, ORDER), f32),
            jax.ShapeDtypeStruct((16, ORDER), f32),
            jax.ShapeDtypeStruct((2, TERMS), f32),
        ),
        in_specs=[pl.BlockSpec(memory_space=pltpu.HBM)] * 4,
        out_specs=(vmem, vmem, vmem),
        scratch_shapes=[
            pltpu.VMEM((2 * DEPTH, ORDER), jnp.bfloat16),
            *[pltpu.VMEM((2, 256, 3 * DEPTH), jnp.bfloat16)] * 4,
            pltpu.VMEM((2, 256, 128), f32),
            pltpu.VMEM((4, 4, 4, 256, 128), f32),
            pltpu.VMEM((4, 4, 4, 256, 128), f32),
            pltpu.VMEM((4, 4, 4, 256, 128), f32),
            pltpu.VMEM((3, 4, 4, 256, 128), f32),
            pltpu.VMEM((3, 4, 256, 128), f32),
            pltpu.VMEM((3, 256, 128), f32),
            pltpu.VMEM((128, 256), f32),
            pltpu.VMEM((16, 16, 128), f32),
            pltpu.VMEM((8, 16, 256), f32),
            pltpu.VMEM((4, 256, TERMS_PAD), f32),
            pltpu.VMEM((384, TERMS_PAD), jnp.bfloat16),
            pltpu.VMEM((1, TERMS_PAD), f32),
            pltpu.VMEM((16, 1, TERMS_PAD), f32),
            pltpu.VMEM((8, 1, TERMS_PAD), f32),
            pltpu.VMEM((1, TERMS), jnp.int32),
            pltpu.VMEM((1, TERMS), jnp.int32),
            pltpu.VMEM((1, TERMS), jnp.int32),
            dma((11,)),
            dma((1,)),
            dma((17,)),
            dma((1,)),
            dma((32,)),
            dma((24,)),
            dma((1,)),
            dma((3, 4)),
            dma((3, 4)),
            dma((1,)),
            dma((3,)),
            dma((1,)),
            dma((1,)),
            dma((1,)),
            dma((1,)),
            dma((2,)),
            dma((2,)),
        ],
        compiler_params=pltpu.CompilerParams(
            collective_id=0, has_side_effects=True, vmem_limit_bytes=50 * 1024 * 1024
        ),
    )(*(pltpu.with_memory_space_constraint(v, pltpu.HBM) for v in (amplitudes, pauli_x.reshape(1, TERMS), pauli_z.reshape(1, TERMS), pauli_phase.reshape(1, TERMS))))
    return pl.pallas_call(
        put_out,
        out_shape=tuple(jax.ShapeDtypeStruct(r.shape, f32) for r in results),
        in_specs=[vmem] * 3,
        out_specs=(vmem,) * 3,
        compiler_params=pltpu.CompilerParams(vmem_limit_bytes=4 * 1024 * 1024),
    )(*results)


def solution(mesh):
    finer = Mesh(mesh.devices.reshape(mesh.shape["gx"], 2, 2, 4, 2), AXES)
    return jax.shard_map(
        on_device,
        mesh=finer,
        in_specs=(P(None, AXES, None), P(), P(), P()),
        out_specs=(P(AXES, None), P(AXES, None), P()),
        check_vma=False,
    )
```

```python
import functools

import jax
import jax.numpy as jnp
from jax import lax
from jax.experimental import pallas as pl
from jax.experimental.pallas import tpu as pltpu
from jax.sharding import Mesh
from jax.sharding import PartitionSpec as P

ORDER = 2048
COLS = 65536
DEPTH = 512
TERMS = 200
TERMS_PAD = 256
AXES = ("gx", "gy_0", "gy_1", "gz_0", "gz_1")
ROWS = (slice(0, 88), slice(88, 176), slice(176, 256))
FAR, PURE, ACC = 0, 1, 2
LAG_Z, LAG_XY = 4, 4
BASE = (0, 8, 16)
TAKE = (0, 4, 8)
UNITS = (
    (2, 2), (2, 3), (3, 2), (2, 1), (1, 2), (3, 3), (3, 1), (1, 3),
    (1, 1), (2, 0), (3, 0), (1, 0), (0, 2), (0, 3), (0, 1), (0, 0),
)
LO, HI = slice(0, 2), slice(2, 4)
HALF = (LO, HI)


def remote(src, dst, send, recv, device):
    return pltpu.make_async_remote_copy(
        src_ref=src,
        dst_ref=dst,
        send_sem=send,
        recv_sem=recv,
        device_id=device,
        device_id_type=pl.DeviceIdType.MESH,
    )


def parity(values):
    values = values ^ (values >> 8)
    values = values ^ (values >> 4)
    values = values ^ (values >> 2)
    values = values ^ (values >> 1)
    return values & 1


def kernel(
    amp, px_in, pz_in, pph_in,
    out_re, out_im, out_ex,
    s, t0, t1, t2, t3, lower, p, stage, cross, ph1, ph2, ph3, flipped, direct, mirror, weights, pick, shares, part0, part1,
    px, pz, pph, in_sem, core_ss, core_rs, ss1, far1, take_s, ss2, far2, take2_s, ss3, rs3,
    dss, drs, mss, mrs, ess, ers,
):
    x0 = lax.axis_index("gx")
    zh = lax.axis_index("gy_0")
    core = lax.axis_index("gy_1")
    y0 = lax.axis_index("gz_0")
    zl = lax.axis_index("gz_1")
    z0 = 2 * zh + zl
    me = x0 * 32 + zh * 16 + core * 8 + y0 * 2 + zl

    def at_x(step):
        return {"gx": lax.rem(x0 + step, 4)}

    def at_y(step):
        return {"gz_0": lax.rem(y0 + step, 4)}

    def at_z(step):
        z = lax.rem(z0 + step, 4)
        return {"gy_0": z // 2, "gz_1": lax.rem(z, 2)}

    along = (at_x, at_y, at_z)
    along2 = (at_y, at_z, at_x)
    along3 = (at_z, at_x, at_y)
    origin2 = (y0, z0, x0)
    origin3 = (z0, x0, y0)
    other_core = {"gy_1": 1 - core}

    def block_of(slot, y):
        return 4 * (core + slot - 2 * core * slot) + lax.rem(y + 1, 4)


    flips = (t0, t1, t2, t3)

    def at_offset(off_y):
        return lax.rem(y0 + off_y, 4)

    def transposed(slot, off_y):
        t = flips[off_y]
        first = pl.multiple_of(block_of(slot, at_offset(off_y)) * 256, 256)
        re_t = s[:DEPTH, pl.ds(first, 256)].T
        im_t = s[DEPTH:, pl.ds(first, 256)].T
        t[slot, :, :DEPTH] = re_t
        t[slot, :, DEPTH : 2 * DEPTH] = im_t
        t[slot, :, 2 * DEPTH :] = -re_t

    def factor(slot, off_y, imag):
        return flips[off_y][slot, :, pl.ds(pl.multiple_of(imag * DEPTH, DEPTH), 2 * DEPTH)]

    def column(col):
        return s[:, pl.ds(pl.multiple_of(col * 256, 256), 256)]

    dot = functools.partial(jnp.dot, preferred_element_type=jnp.float32)

    def half_product(slot, dst, off_y, x, half):
        y = at_offset(off_y)
        block, col = block_of(slot, y), 2 * x + half
        value = dot(factor(slot, off_y, (block - col + 7) // 8), column(col))
        for k in range(2):
            dst[y, x, 2 * half + k] = value[:, 128 * k : 128 * k + 128]

    def products(off_y, x):
        y = at_offset(off_y)
        for half in range(2):
            col = 2 * x + half
            left = jnp.concatenate(
                [
                    factor(slot, off_y, (block_of(slot, y) - col + 7) // 8)
                    for slot in range(2)
                ],
                axis=0,
            )
            value = dot(left, column(col))
            for slot, dst in ((0, stage), (1, p)):
                for k in range(2):
                    dst[y, x, 2 * half + k] = value[
                        256 * slot : 256 * slot + 256, 128 * k : 128 * k + 128
                    ]

    def diagonal(slot, off_y):
        imag = dot(factor(slot, off_y, 1), column(block_of(slot, at_offset(off_y))))
        for k in range(2):
            lower[k] = imag[:, 128 * k : 128 * k + 128]

    def mend(y, x, slots=(0, 1)):
        row = lax.broadcasted_iota(jnp.int32, (256, 128), 0)
        lane = lax.broadcasted_iota(jnp.int32, (256, 128), 1)
        for slot in slots:
            dst = p if slot else stage
            block = block_of(slot, y)

            @pl.when(block // 2 == x)
            def _(dst=dst, block=block):
                for k in range(2):
                    z = 2 * lax.rem(block, 2) + k
                    dst[y, x, z] = jnp.where(lane + 128 * k >= row, dst[y, x, z], lower[k])

    def unit(v, beside=lambda: None):
        off_y, _, y, x = unit_of(v)
        shift = block_of(0, y) // 2 - x

        @pl.when(lax.rem(shift + 4, 2) == 0)
        def _():
            products(off_y, x)
            diagonal(lax.rem(shift + 4, 4) // 2, off_y)
            beside()

        @pl.when(lax.rem(shift + 4, 2) != 0)
        def _():
            products(off_y, x)
            beside()

        mend(y, x)
        if v:
            core_copy(v, y, x).start()

    def unit_of(v):
        off_y, off_x = UNITS[v]
        return off_y, off_x, lax.rem(y0 + off_y, 4), lax.rem(x0 + off_x, 4)

    def core_copy(v, y, x):
        return remote(stage.at[y, x], cross.at[y, x], core_ss.at[0], core_rs.at[v], other_core)

    def core_half(y, x, half):
        return remote(
            stage.at[y, x, HALF[half]], cross.at[y, x, HALF[half]],
            core_ss.at[0], core_rs.at[16 * half], other_core,
        )

    def copy1(kind, o, src, key, index, step):
        line = index // 2 if o < 2 else index
        return remote(
            src,
            ph1.at[(kind,) + key + (ROWS[o],)],
            ss1.at[0],
            far1.at[BASE[o] + index] if kind == FAR else take_s.at[TAKE[o] + line],
            along[o](step),
        )

    def send1(kind, o, src, key, index, step):
        copy1(kind, o, src, key, index, step).start()

    def wait1(o, key, index):
        copy1(FAR, o, ph1.at[(FAR,) + key + (ROWS[o],)], key, index, 1).wait_recv()

    def add_cross(y, x):
        for z in range(4):
            p[y, x, z] += cross[y, x, z]

    def finish(v):
        off_y, off_x, y, x = unit_of(v)
        for o, off, line in ((0, off_x, y), (1, off_y, x)):
            @pl.when(off == 2)
            def _(o=o, line=line):
                for h, step in ((0, 1), (1, 3)):
                    send1(FAR, o, p.at[y, x, HALF[h], ROWS[o]], (line, HALF[h]), 2 * line + h, step)

            @pl.when(off == 1)
            def _(o=o, line=line):
                send1(PURE, o, p.at[y, x, HI, ROWS[o]], (line, HI), 2 * line + 1, 1)

            @pl.when(off == 3)
            def _(o=o, line=line):
                send1(PURE, o, p.at[y, x, LO, ROWS[o]], (line, LO), 2 * line, 3)

        up = v % 2
        far, right, left = (lax.rem(z0 + k, 4) for k in (2, 1, 3))

        @pl.when(up == 0)
        def _():
            send1(FAR, 2, p.at[y, x, far, ROWS[2]], (y, x), 4 * y + x, 1)
            send1(PURE, 2, p.at[y, x, left, ROWS[2]], (y, x), 4 * y + x, 3)

        @pl.when(up == 1)
        def _():
            send1(FAR, 2, p.at[y, x, far, ROWS[2]], (y, x), 4 * y + x, 3)
            send1(PURE, 2, p.at[y, x, right, ROWS[2]], (y, x), 4 * y + x, 1)

    def forward_xy(v):
        off_y, off_x, y, x = unit_of(v)
        for o, off, line in ((0, off_x, y), (1, off_y, x)):
            for h, step in ((0, 1), (1, 3)):
                @pl.when(off == step)
                def _(o=o, line=line, h=h, step=step):
                    key, index = (line, HALF[h]), 2 * line + h
                    wait1(o, key, index)
                    p[y, x, HALF[h], ROWS[o]] += ph1[FAR, line, HALF[h], ROWS[o]]
                    send1(ACC, o, p.at[y, x, HALF[h], ROWS[o]], key, index, step)

    def forward_z(v):
        _, _, y, x = unit_of(v)
        wait1(2, (y, x), 4 * y + x)
        for h, step in ((0, 1), (1, 3)):
            @pl.when(v % 2 == h)
            def _(step=step):
                z = lax.rem(z0 + step, 4)
                p[y, x, z, ROWS[2]] += ph1[FAR, y, x, ROWS[2]]
                send1(ACC, 2, p.at[y, x, z, ROWS[2]], (y, x), 4 * y + x, step)

    def held(o, b, cs):
        if o == 0:
            return (b, x0, cs, ROWS[0])
        if o == 1:
            return (y0, cs, b, ROWS[1])
        return (cs, b, z0, ROWS[2])

    def landed(o, b, cs):
        return (b, cs, ROWS[0]) if o == 0 else (cs, b, ROWS[o])

    def at2(o, k):
        return lax.rem(origin2[o] + k, 4)

    def at3(o, k):
        return lax.rem(origin3[o] + k, 4)

    groups = ((((LO, 0, 0), (HI, 1, 1)),) + tuple(
        tuple((at3(o, k), n % 2, n) for n, k in enumerate((2, 3, 1, 0))) for o in (1, 2)
    ))

    def arrived(o, line):
        key = (line // 4, lax.rem(line, 4)) if o == 2 else (line, slice(None))
        ref = ph1.at[(slice(PURE, ACC + 1),) + key + (ROWS[o],)]
        remote(ref, ref, ss1.at[0], take_s.at[TAKE[o] + line], other_core).wait_recv()

    def add1(o, b, c):
        p[held(o, b, c)] += ph1[(PURE,) + landed(o, b, c)] + ph1[(ACC,) + landed(o, b, c)]

    def take0(b):
        arrived(0, b)
        for c in range(4):
            add1(0, b, c)

    def copy2(kind, o, src, group, step):
        cs, _, n = group
        return remote(
            src, ph2.at[kind, cs, ROWS[o]], ss2.at[0],
            far2.at[o, n] if kind == FAR else take2_s.at[o, n if o else 0], along2[o](step),
        )

    def wait2(o, group):
        copy2(FAR, o, ph2.at[FAR, group[0], ROWS[o]], group, 1).wait_recv()

    def send2(kind, o, group, step):
        b = at2(o, 2 if kind == FAR else step)
        copy2(kind, o, p.at[held(o, b, group[0])], group, step).start()

    UP = (1, 3)
    DOWN = (3, 1)

    def accumulate2(o, n):
        group = groups[o][n]
        cs, h, _ = group
        wait2(o, group)
        p[held(o, at2(o, UP[h]), cs)] += ph2[FAR, cs, ROWS[o]]
        send2(ACC, o, group, UP[h])

    def far0():
        take0(at2(0, 2))
        for group in groups[0]:
            send2(FAR, 0, group, UP[group[1]])

    def pure0(step):
        take0(at2(0, step))
        for group in groups[0]:
            if DOWN[group[1]] == step:
                send2(PURE, 0, group, step)

    def open2(o, n):
        group = groups[o][n]
        cs, h, _ = group

        def take(k):
            b = at2(o, k)
            if o == 2:
                arrived(2, 4 * cs + b)
            add1(o, b, cs)

        if o == 1:
            arrived(1, cs)
        take(2)
        send2(FAR, o, group, UP[h])
        take(DOWN[h])
        send2(PURE, o, group, DOWN[h])
        take(UP[h])

    def direct2(o, n):
        c = groups[o][n][0]
        if o == 1:
            arrived(1, c)
        for k in (2, 1, 3):
            b = at2(o, k)
            if o == 2:
                arrived(2, 4 * c + b)
            add1(o, b, c)
            remote(
                p.at[held(o, b, c)], ph2.at[k - 1, c, ROWS[o]],
                ss2.at[0], take2_s.at[o, n], along2[o](k),
            ).start()

    def own(o, c):
        return held(o, origin2[o], c)

    def send3(o, k):
        remote(
            p.at[own(o, at3(o, k))], ph3.at[k - 1, ROWS[o]], ss3.at[0], rs3.at[o], along3[o](k)
        ).start()

    def close2(o, n):
        c = groups[o][n][0]
        if o == 2:
            arrived(2, 4 * c + x0)
        add1(o, origin2[o], c)
        kinds = slice(PURE if n < 2 else FAR, ACC + 1)
        ref = ph2.at[kinds, c, ROWS[o]]
        remote(ref, ref, ss2.at[0], take2_s.at[o, n], other_core).wait_recv()
        total = ph2[PURE, c, ROWS[o]] + ph2[ACC, c, ROWS[o]]
        if n == 2:
            total = total + ph2[FAR, c, ROWS[o]]
        p[own(o, c)] += total
        send3(o, (2, 3, 1)[n])

    def close0():
        take0(y0)
        ref = ph2.at[PURE : ACC + 1, :, ROWS[0]]
        remote(ref, ref, ss2.at[0], take2_s.at[0, 0], other_core).wait_recv()
        for k in (2, 1, 3, 0):
            c = at3(0, k)
            p[own(0, c)] += ph2[PURE, c, ROWS[0]] + ph2[ACC, c, ROWS[0]]
            if k:
                send3(0, k)

    def share(pieces, first=False):
        runs = []
        for o, c in pieces:
            run = p[own(o, c)]
            row = ROWS[o].start + lax.broadcasted_iota(jnp.int32, run.shape, 0)
            lane = lax.broadcasted_iota(jnp.int32, run.shape, 1)
            runs.append((o, c, run, row, lane))
        moved = jnp.concatenate([run[2] for run in runs], axis=0)
        row = jnp.concatenate([run[3] for run in runs], axis=0)
        lane = jnp.concatenate([run[4] for run in runs], axis=0)
        for bit in range(7):
            hop = 1 << bit
            swapped = jnp.where(
                (lane & hop) != 0, pltpu.roll(moved, hop, 1), pltpu.roll(moved, 128 - hop, 1)
            )
            moved = jnp.where((row & hop) != 0, swapped, moved)
        high = moved.astype(jnp.bfloat16)
        rest = moved - high.astype(jnp.float32)
        middle = rest.astype(jnp.bfloat16)
        low = (rest - middle.astype(jnp.float32)).astype(jnp.bfloat16)
        read = dot(jnp.concatenate([high, middle, low], axis=1), pick[:, :TERMS])
        weight = jnp.concatenate([weights[c, ROWS[o], :TERMS] for o, c in pieces], axis=0)
        total = jnp.sum(weight * read, axis=0, keepdims=True)
        shares[:, :TERMS] = total if first else shares[:, :TERMS] + total

    def load(q):
        columns = pl.ds(pl.multiple_of(512 * q, 512), 512)
        return [
            pltpu.make_async_copy(
                amp.at[k, :, columns], s.at[pl.ds(DEPTH * k, DEPTH), columns], in_sem.at[2 * q + k]
            )
            for k in range(2)
        ]

    def start(q):
        for copy in load(q):
            copy.start()

    def loaded(q):
        for copy in load(q):
            copy.wait()

    first_y, first_x = lax.rem(y0 + 2, 4), lax.rem(x0 + 2, 4)
    chunk = block_of(0, first_y) // 2
    later = [lax.rem(chunk + k, 4) for k in (2, 1, 3)]
    start(chunk)
    pl.when(first_x != chunk)(lambda: start(first_x))
    for q in later:
        pl.when(first_x != q)(lambda q=q: start(q))
    terms = [
        pltpu.make_async_copy(src, dst, in_sem.at[8 + n])
        for n, (src, dst) in enumerate(((px_in, px), (pz_in, pz), (pph_in, pph)))
    ]
    for copy in terms:
        copy.start()
    barrier = pltpu.get_barrier_semaphore()
    partners = [other_core] + [f(k) for f in along for k in (1, 3)]
    for device in partners:
        pl.semaphore_signal(barrier, inc=1, device_id=device, device_id_type=pl.DeviceIdType.MESH)
    loaded(chunk)
    pl.when(first_x != chunk)(lambda: loaded(first_x))

    _, _, y, x = unit_of(0)
    transposed(0, 2)
    half_product(0, stage, 2, x, 0)
    half_product(0, stage, 2, x, 1)
    pl.when(block_of(0, y) // 2 == x)(lambda: diagonal(0, 2))
    mend(y, x, (0,))
    pl.semaphore_wait(barrier, len(partners))
    for half in range(2):
        core_half(y, x, half).start()
    for q in later:
        pl.when(first_x != q)(lambda q=q: loaded(q))
    for copy in terms:
        copy.wait()
    transposed(1, 2)
    half_product(1, p, 2, x, 0)
    half_product(1, p, 2, x, 1)
    pl.when(block_of(1, y) // 2 == x)(lambda: diagonal(1, 2))
    mend(y, x, (1,))

    def turned(off_y):
        for slot in range(2):
            transposed(slot, off_y)

    unit(1, lambda: turned(3))

    def settle(v):
        _, _, y, x = unit_of(v)
        core_copy(v, y, x).wait_recv()
        add_cross(y, x)
        finish(v)

    for half in range(2):
        core_half(y, x, half).wait_recv()
    add_cross(y, x)
    finish(0)
    unit(2)

    for u in range(3, 16):
        _, _, last_y, last_x = unit_of(u - 2)
        core_copy(u - 2, last_y, last_x).wait_recv()

        def beside(u=u, last_y=last_y, last_x=last_x):
            add_cross(last_y, last_x)
            if u in (3, 7):
                turned(1 if u == 3 else 0)

        unit(u, beside)
        finish(u - 2)
        if u >= 2 + LAG_Z:
            forward_z(u - 2 - LAG_Z)
        if u >= 2 + LAG_XY:
            forward_xy(u - 2 - LAG_XY)
        if u == 13:
            open2(2, 0)
        if u == 14:
            far0()

    settle(14)
    forward_z(10)
    forward_xy(10)
    row_block = block_of(1, y0)
    col_block = 4 * x0 + z0
    xs, zs, phase = px[...], pz[...], pph[...]
    even = parity(xs & zs) == 0
    for n in range(3):
        rows = slice(128 * n, 128 * n + 128)
        pick[rows, :TERMS] = jnp.where(
            lax.broadcasted_iota(jnp.int32, (128, TERMS), 0) == (xs & 127), 1.0, 0.0
        ).astype(jnp.bfloat16)
    count = jnp.where(xs == 0, 1.0, 2.0) * (1.0 / COLS)
    row = lax.broadcasted_iota(jnp.int32, (256, TERMS), 0)
    for c in range(4):
        cols = jnp.where(row < 88, 4 * x0 + c, jnp.where(row < 176, 4 * c + z0, col_block))
        rows = 256 * jnp.where(row < 176, row_block, block_of(1, c)) + row
        sign = jnp.where(parity(rows & zs) == 0, count, -count)
        keep = ((rows ^ xs) >> 7) == cols
        weights[c, :, :TERMS] = jnp.where(
            keep & (((rows ^ xs) >= rows) == even), sign, 0.0
        )

    def phased(share):
        phase_re = jnp.where(phase == 0, 1.0, jnp.where(phase == 2, -1.0, 0.0))
        phase_im = jnp.where(phase == 1, 1.0, jnp.where(phase == 3, -1.0, 0.0))
        return share * jnp.concatenate(
            [jnp.where(even, phase_re, -phase_im), jnp.where(even, phase_im, phase_re)], axis=0
        )
    settle(15)
    forward_z(11)
    forward_xy(11)
    forward_z(12)
    pure0(3)
    open2(1, 0)
    forward_z(13)
    forward_xy(13)
    accumulate2(2, 0)
    open2(2, 1)
    open2(1, 1)
    forward_z(14)
    forward_xy(14)
    forward_z(15)
    pure0(1)
    direct2(2, 2)
    direct2(1, 2)
    accumulate2(1, 0)
    accumulate2(2, 1)
    accumulate2(0, 1)
    accumulate2(0, 0)
    accumulate2(1, 1)
    close2(2, 0)
    direct2(2, 3)
    direct2(1, 3)
    close2(2, 1)
    close2(1, 0)
    close2(2, 2)
    close2(1, 1)
    close2(1, 2)
    share([(o, at3(o, k)) for o in (1, 2) for k in (2, 3, 1)], True)
    close0()
    for o in (1, 2):
        c = origin3[o]
        if o == 2:
            arrived(2, 4 * c + x0)
        add1(o, origin2[o], c)
        ref = ph2.at[:, c, ROWS[o]]
        remote(ref, ref, ss2.at[0], take2_s.at[o, 3], other_core).wait_recv()
        p[own(o, c)] += ph2[0, c, ROWS[o]] + ph2[1, c, ROWS[o]] + ph2[2, c, ROWS[o]]

    share([(0, c) for c in range(4)] + [(o, at3(o, 0)) for o in (1, 2)])
    here = shares[:, :TERMS]

    def give(here, parts, n, mine, count, where):
        parts[mine, :, :TERMS] = here
        for k in range(1, count):
            remote(
                parts.at[mine], parts.at[mine], ess.at[n], ers.at[n],
                where(lax.rem(mine + k, count)),
            ).start()

    def collect(parts, n, count):
        rest = parts.at[pl.ds(0, count - 1)]
        remote(rest, rest, ess.at[n], ers.at[n], other_core).wait_recv()
        total = parts[0, :, :TERMS]
        for k in range(1, count):
            total = total + parts[k, :, :TERMS]
        return total

    give(
        here, part1, 1, 2 * y0 + core, 8, lambda k: {"gz_0": k // 2, "gy_1": lax.rem(k, 2)}
    )

    for o in range(3):
        ref = ph3.at[:, ROWS[o]]
        remote(ref, ref, ss3.at[0], rs3.at[o], other_core).wait_recv()
    block = p[y0, x0, z0] + ph3[0] + ph3[1] + ph3[2]
    p[y0, x0, z0] = block


    def device(e):
        return {
            "gx": e // 32,
            "gy_0": lax.rem(e // 16, 2),
            "gy_1": lax.rem(e // 8, 2),
            "gz_0": lax.rem(e // 2, 4),
            "gz_1": lax.rem(e, 2),
        }

    def direct_copy(k):
        e = 16 * row_block + k
        return e, remote(
            p.at[y0, x0, z0, pl.ds(16 * k, 16)], direct.at[col_block],
            dss.at[0], drs.at[0], device(e),
        )

    def mirror_copy(k):
        e = 8 * col_block + k
        return e, remote(
            flipped.at[pl.ds(16 * k, 16)], mirror.at[row_block],
            mss.at[0], mrs.at[0], device(e),
        )

    far_first = [
        8 * half + 2 * lax.rem(y0 + k, 4) + low
        for half in range(2) for k in (2, 3, 1, 0) for low in range(2)
    ]
    @pl.when(me // 16 != row_block)
    def _():
        for k in far_first:
            direct_copy(k)[1].start()

    @pl.when(me // 16 == row_block)
    def _():
        for k in range(16):
            e, copy = direct_copy(k)
            pl.when(e != me)(copy.start)

            @pl.when(e == me)
            def _(k=k):
                direct[col_block] = p[y0, x0, z0, pl.ds(16 * k, 16)]


    give(
        collect(part1, 1, 8), part0, 0, 4 * x0 + z0, 16,
        lambda k: {"gx": k // 4, "gy_0": lax.rem(k // 2, 2), "gz_1": lax.rem(k, 2)},
    )
    flipped[...] = block.T

    @pl.when(me // 8 != col_block)
    def _():
        for k in far_first[:8]:
            mirror_copy(k)[1].start()

    @pl.when(me // 8 == col_block)
    def _():
        for k in range(8):
            e, copy = mirror_copy(k)
            pl.when(e != me)(copy.start)

            @pl.when(e == me)
            def _(k=k):
                mirror[row_block] = flipped[pl.ds(16 * k, 16)]
    out_ex[...] = phased(collect(part0, 0, 16))

    def landed_and_left(ref, ss, rs):
        copy = remote(ref, ref, ss, rs, other_core)
        copy.wait_recv()
        copy.wait_send()

    @pl.when(me // 16 == row_block)
    def _():
        landed_and_left(direct.at[pl.ds(0, 15)], dss.at[0], drs.at[0])

    @pl.when(me // 16 != row_block)
    def _():
        landed_and_left(direct, dss.at[0], drs.at[0])

    @pl.when(me // 8 == col_block)
    def _():
        landed_and_left(mirror.at[pl.ds(0, 7)], mss.at[0], mrs.at[0])

    @pl.when(me // 8 != col_block)
    def _():
        landed_and_left(mirror, mss.at[0], mrs.at[0])

    row = 16 * me + lax.broadcasted_iota(jnp.int32, (16, 128), 0)
    lane = lax.broadcasted_iota(jnp.int32, (16, 128), 1)
    for k in range(16):
        given = direct[k] * (1.0 / COLS)
        turned = mirror[k // 2, :, 128 * (k % 2) : 128 * (k % 2) + 128] * (1.0 / COLS)
        col = 128 * k + lane
        out_re[:, 128 * k : 128 * k + 128] = jnp.where(col >= row, given, turned)
        out_im[:, 128 * k : 128 * k + 128] = jnp.where(
            col < row, given, jnp.where(col == row, 0.0, -turned)
        )

    def left(ref, sem):
        remote(ref, ref, sem, core_rs.at[0], other_core).wait_send()

    left(stage, core_ss.at[0])
    left(ph1, ss1.at[0])
    left(ph2, ss2.at[0])
    left(ph3, ss3.at[0])
    left(part0.at[pl.ds(0, 15)], ess.at[0])
    left(part1.at[pl.ds(0, 7)], ess.at[1])


def put_out(re, im, ex, out_re, out_im, out_ex):
    out_re[...] = re[...]
    out_im[...] = im[...]
    out_ex[...] = ex[...]


def on_device(amplitudes, pauli_x, pauli_z, pauli_phase):
    vmem = pl.BlockSpec(memory_space=pltpu.VMEM)
    f32 = jnp.float32
    dma = pltpu.SemaphoreType.DMA
    results = pl.pallas_call(
        kernel,
        out_shape=(
            jax.ShapeDtypeStruct((16, ORDER), f32),
            jax.ShapeDtypeStruct((16, ORDER), f32),
            jax.ShapeDtypeStruct((2, TERMS), f32),
        ),
        in_specs=[pl.BlockSpec(memory_space=pltpu.HBM)] * 4,
        out_specs=(vmem, vmem, vmem),
        scratch_shapes=[
            pltpu.VMEM((2 * DEPTH, ORDER), jnp.bfloat16),
            *[pltpu.VMEM((2, 256, 3 * DEPTH), jnp.bfloat16)] * 4,
            pltpu.VMEM((2, 256, 128), f32),
            pltpu.VMEM((4, 4, 4, 256, 128), f32),
            pltpu.VMEM((4, 4, 4, 256, 128), f32),
            pltpu.VMEM((4, 4, 4, 256, 128), f32),
            pltpu.VMEM((3, 4, 4, 256, 128), f32),
            pltpu.VMEM((3, 4, 256, 128), f32),
            pltpu.VMEM((3, 256, 128), f32),
            pltpu.VMEM((128, 256), f32),
            pltpu.VMEM((16, 16, 128), f32),
            pltpu.VMEM((8, 16, 256), f32),
            pltpu.VMEM((4, 256, TERMS_PAD), f32),
            pltpu.VMEM((384, TERMS_PAD), jnp.bfloat16),
            pltpu.VMEM((1, TERMS_PAD), f32),
            pltpu.VMEM((16, 1, TERMS_PAD), f32),
            pltpu.VMEM((8, 1, TERMS_PAD), f32),
            pltpu.VMEM((1, TERMS), jnp.int32),
            pltpu.VMEM((1, TERMS), jnp.int32),
            pltpu.VMEM((1, TERMS), jnp.int32),
            dma((11,)),
            dma((1,)),
            dma((17,)),
            dma((1,)),
            dma((32,)),
            dma((24,)),
            dma((1,)),
            dma((3, 4)),
            dma((3, 4)),
            dma((1,)),
            dma((3,)),
            dma((1,)),
            dma((1,)),
            dma((1,)),
            dma((1,)),
            dma((2,)),
            dma((2,)),
        ],
        compiler_params=pltpu.CompilerParams(
            collective_id=0, has_side_effects=True, vmem_limit_bytes=50 * 1024 * 1024
        ),
    )(*(pltpu.with_memory_space_constraint(v, pltpu.HBM) for v in (amplitudes, pauli_x.reshape(1, TERMS), pauli_z.reshape(1, TERMS), pauli_phase.reshape(1, TERMS))))
    return pl.pallas_call(
        put_out,
        out_shape=tuple(jax.ShapeDtypeStruct(r.shape, f32) for r in results),
        in_specs=[vmem] * 3,
        out_specs=(vmem,) * 3,
        compiler_params=pltpu.CompilerParams(vmem_limit_bytes=4 * 1024 * 1024),
    )(*results)


def solution(mesh):
    finer = Mesh(mesh.devices.reshape(mesh.shape["gx"], 2, 2, 4, 2), AXES)
    return jax.shard_map(
        on_device,
        mesh=finer,
        in_specs=(P(None, AXES, None), P(), P(), P()),
        out_specs=(P(AXES, None), P(AXES, None), P()),
        check_vma=False,
    )
```
